32 devices in a mesh: groups: 2 (over x), ctx: 16 (over z, y, core).
Axes of the slice: x: 2, y: 2, z: 4, core: 2. Of those that a mesh axis runs over, the one named last changes fastest.
Arguments:
- queries: bfloat16 [512, 128, 576], P(('groups', 'ctx')), parts along dimension 0, may hold values from -4 to 4
- latent_cache: bfloat16 [32768, 576], P(('groups', 'ctx')), parts along dimension 0, may hold values from -4 to 4
- block_picks: int32 [32, 32], P(('groups', 'ctx')), parts along dimension 0, may hold values from 0 to 255, as said below
- lengths: int32 [512], P(('groups', 'ctx')), parts along dimension 0, may hold values from 8192 to 16384
Outputs:
- latent_out: bfloat16 [512, 128, 512], P(('groups', 'ctx')), parts along dimension 0
The draws below stay inside these ranges and needn't reach their ends.
There are 2 independent parts, one for each index of `groups`. The reference program is written for one: setup_inputs(seed, part) draws one part's arguments, and reference() takes and returns one part's arrays. A program takes and returns all parts, laid end to end along the dimension named above; each array names one. Nothing has to cross between parts.
Inputs may be any that keep to these rules, and one draw needn't show every extreme that they name: `block_picks`: each row names 32 different blocks. At most 4 of a row's blocks lie in one owner's range of 16 consecutive blocks, and every row reaches this with its first 4 entries, which lie in the first half of the context. Over all rows together at most 8 different blocks of one owner's range are named, and some owner reaches this.
All inputs are finite; a program needn't handle non-finite values.
Results may differ from the reference program's by a relative error of at most 0.0035.
Values may be sent and summed in bfloat16 or wider, within the bound.
A program may use at most 128 MiB of HBM per device.

```python
import jax
import jax.numpy as jnp
from jax import lax

H = 128
LAT = 512
BLOCK = 64
TOPK = 32
BLK_DEV = 16
WIDTH = 576
CONTEXT = 16384
QROWS = 256
N_CTX = 16


def draw_latent_cache(key, part):
    seed_cache = jax.random.fold_in(key, 21)
    values = jnp.clip(jax.random.normal(seed_cache, (CONTEXT, WIDTH), jnp.float32), -4.0, 4.0)
    return values.astype(jnp.bfloat16)


def draw_block_picks(key, part):
    capacity = max(1, 2 * TOPK // N_CTX)
    pair_count = N_CTX * capacity
    starting_picks = jax.random.fold_in(key, 41)
    popular_region_seed, extra_credit_seed, noise_perturbation_seed, permutation_seed, split_choice_seed = jax.random.split(starting_picks, 5)
    hot_owner = jax.random.randint(popular_region_seed, (N_CTX,), 0, max(1, N_CTX // 2))
    hot_owner = hot_owner.at[1].set(hot_owner[0])
    owner_preference_lift = jax.random.randint(extra_credit_seed, (N_CTX,), 0, 2) * 4096
    jitter_amount = jax.random.randint(noise_perturbation_seed, (N_CTX, pair_count), 0, 4096)
    pair_index = jnp.arange(pair_count, dtype=jnp.int32)
    every_pair_holder = pair_index // capacity
    required_blocks = (every_pair_holder[None, :] == hot_owner[:, None]).astype(jnp.int32) * 16384
    block_ratings = jitter_amount + owner_preference_lift[every_pair_holder][None, :] + required_blocks
    block_ratings = block_ratings * pair_count + pair_index[None, :]
    _, chosen = lax.top_k(block_ratings, TOPK)
    pair_owner = chosen // capacity
    pair_slot = chosen % capacity
    ranks = jax.random.randint(permutation_seed, (N_CTX, BLK_DEV), 0, 65536) * BLK_DEV + jnp.arange(BLK_DEV, dtype=jnp.int32)[None, :]
    candidates = jnp.argsort(ranks, axis=1)[:, :2 * capacity].astype(jnp.int32)
    side_bit = jax.random.randint(split_choice_seed, (N_CTX, TOPK), 0, 2)
    group_index = jnp.arange(N_CTX, dtype=jnp.int32)[:, None]
    at_shared = pair_owner == hot_owner[0]
    side_bit = jnp.where((group_index == 0) & at_shared, 0, side_bit)
    side_bit = jnp.where((group_index == 1) & at_shared, 1, side_bit)
    local_block = candidates[pair_owner, 2 * pair_slot + side_bit]
    return (pair_owner * BLK_DEV + local_block).astype(jnp.int32)


def draw_queries(key, part):
    seed_rows = jax.random.fold_in(key, 31)
    array_shape = (QROWS, H, WIDTH)
    values = jnp.clip(jax.random.normal(seed_rows, array_shape, jnp.float32), -4.0, 4.0)
    return values.astype(jnp.bfloat16)


def plant(values, key, least, top_value):
    extent = values.shape
    spot = [jax.random.randint(jax.random.fold_in(key, axis), (), 0, extent[axis]) for axis in range(len(extent))]
    values = values.at[tuple(spot)].set(least)
    longest = extent.index(max(extent))
    spot[longest] = (spot[longest] + 1) % extent[longest]
    return values.at[tuple(spot)].set(top_value)


def setup_inputs(seed: int = 0, part: int = 0) -> dict:
    key_of = jax.random.split(jax.random.key(seed), 5)
    part_keys = jax.random.split(jax.random.fold_in(key_of[4], part), 5)
    queries = draw_queries(jax.random.fold_in(jax.random.fold_in(key_of[4], part), 71), part)
    latent_cache = draw_latent_cache(jax.random.fold_in(jax.random.fold_in(key_of[4], part), 71), part)
    block_picks = draw_block_picks(jax.random.fold_in(jax.random.fold_in(key_of[4], part), 71), part)
    lengths = plant(jax.random.randint(part_keys[3], (QROWS,), CONTEXT // 2, CONTEXT + 1), jax.random.fold_in(part_keys[3], 1), CONTEXT // 2, CONTEXT).astype(jnp.int32)
    return dict(queries=queries, latent_cache=latent_cache, block_picks=block_picks, lengths=lengths)


SOFTMAX_SCALE = 192.0 ** -0.5


def attend(query_rows, key_rows, positions, row_lengths):
    total_rows = query_rows.shape[0]
    step_rows = 512 if total_rows % 512 == 0 else total_rows
    block_count = total_rows // step_rows
    latent = key_rows[:, :LAT]

    def per_block(inputs):
        block_queries, block_lengths = inputs
        block_ratings = lax.dot_general(block_queries, key_rows, (((1,), (1,)), ((), ())), preferred_element_type=jnp.float32) * SOFTMAX_SCALE
        visible = positions[None, :] < block_lengths[:, None]
        row_max = jnp.max(jnp.where(visible, block_ratings, -jnp.inf), axis=1, keepdims=True)
        exponent = jnp.where(visible, jnp.exp(block_ratings - row_max), 0.0)
        normaliser = jnp.sum(exponent, axis=1, keepdims=True)
        weights = exponent.astype(jnp.bfloat16)
        result = jnp.dot(weights, latent, preferred_element_type=jnp.float32) / normaliser
        return result.astype(jnp.bfloat16)

    outputs = lax.map(per_block, (query_rows.reshape(block_count, step_rows, query_rows.shape[1]), row_lengths.reshape(block_count, step_rows)))
    return outputs.reshape(total_rows, LAT)


def reference(queries, latent_cache, block_picks, lengths):
    groups = block_picks.shape[0]
    per_group = queries.shape[0] // groups
    head_count = queries.shape[1]
    feature = queries.shape[2]
    within = jnp.arange(BLOCK, dtype=jnp.int32)

    def per_group_attend(group):
        chosen_blocks = lax.dynamic_index_in_dim(block_picks, group, 0, keepdims=False)
        positions = (chosen_blocks[:, None] * BLOCK + within[None, :]).reshape(-1).astype(jnp.int32)
        key_rows = jnp.take(latent_cache, positions, axis=0)
        first_row = (group * per_group).astype(jnp.int32)
        query_rows = lax.dynamic_slice_in_dim(queries, first_row, per_group, 0).reshape(per_group * head_count, feature)
        row_lengths = jnp.repeat(lax.dynamic_slice_in_dim(lengths, first_row, per_group, 0), head_count)
        return attend(query_rows, key_rows, positions, row_lengths)

    outputs = lax.map(per_group_attend, jnp.arange(groups, dtype=jnp.int32))
    return outputs.reshape(queries.shape[0], head_count, LAT)
```

```python
import functools

import jax
import jax.numpy as jnp
from jax import lax
from jax.experimental import pallas as pl
from jax.experimental.pallas import tpu as pltpu
from jax.sharding import PartitionSpec as P

LAT = 512
BLOCK = 64
TOPK = 32
LANES = 128

SOFTMAX_SCALE = 192.0 ** (-0.5)
LOG2E = 1.4426950408889634
MESH = pl.DeviceIdType.MESH
HIDDEN = -1e30


def step_kernel(
    ctx_count, owned, units, picks_ref, lengths_ref, queries_ref, cache_ref, out_ref,
    raw_q, near_cache, q_ref, flags_ref, all_flags, gath, pool, keys_t, values, positions, order,
    top_ref, total_ref, acc_ref, q_sem, cache_sem, flag_send, flag_recv, send, recv,
):
    rows, feature, heads = queries_ref.shape
    rope = feature - LAT
    pair = 2 * BLOCK
    tall = pair * rope // LAT
    line = ctx_count // 4
    late_blocks = 4 * units
    early_blocks = TOPK - late_blocks
    me = lax.axis_index("ctx")
    core = lax.rem(me, 2)
    y = lax.rem(me // 2, 2)
    z = me // 4
    far = jnp.where(2 * z < line, line - 1, 0)

    fetch = pltpu.make_async_copy(queries_ref, raw_q, q_sem)
    fetch_cache = pltpu.make_async_copy(cache_ref, near_cache, cache_sem)
    fetch_cache.start()
    fetch.start()

    def at(zz, yy, cc):
        return (zz * 2 + yy) * 2 + cc

    barrier = pltpu.get_barrier_semaphore()

    @pl.loop(1, ctx_count)
    def _(d):
        pl.semaphore_signal(
            barrier, inc=1, device_id={"ctx": lax.rem(me + d, ctx_count)}, device_id_type=MESH
        )

    flag_rows = flags_ref.shape[0]
    block_id = lax.broadcasted_iota(jnp.int32, (flag_rows, LANES), 0) * LANES
    block_id += lax.broadcasted_iota(jnp.int32, (flag_rows, LANES), 1)
    lane = lax.broadcasted_iota(jnp.int32, (1, LANES), 1)
    flags = jnp.zeros((flag_rows, LANES), jnp.int32)
    ordered = jnp.zeros((1, LANES), jnp.int32)
    early_seen = jnp.int32(0)
    for k in range(TOPK):
        p = picks_ref[0, k]
        owner = p // owned
        is_late = owner // 4 == far
        place = jnp.where(is_late, TOPK - 1 - (k - early_seen), early_seen)
        early_seen += jnp.where(is_late, 0, 1)
        flags = jnp.where(block_id == p, 1, flags)
        ordered = jnp.where(lane == place, p, ordered)
    flags_ref[...] = flags

    pl.semaphore_wait(barrier, ctx_count - 1)

    def flag_copy(d):
        return pltpu.make_async_remote_copy(
            src_ref=flags_ref,
            dst_ref=all_flags.at[me],
            send_sem=flag_send.at[d],
            recv_sem=flag_recv.at[me],
            device_id={"ctx": lax.rem(me + d, ctx_count)},
            device_id_type=MESH,
        )

    def flag_arrival(source):
        return pltpu.make_async_remote_copy(
            src_ref=flags_ref,
            dst_ref=all_flags.at[source],
            send_sem=flag_send.at[0],
            recv_sem=flag_recv.at[source],
            device_id={"ctx": source},
            device_id_type=MESH,
        )

    @pl.loop(1, ctx_count)
    def _(d):
        flag_copy(d).start()

    all_flags[me] = flags

    @pl.loop(1, ctx_count)
    def _(d):
        flag_arrival(lax.rem(me + d, ctx_count)).wait_recv()

    named = jnp.minimum(jnp.max(all_flags[...], axis=0), 1)
    mine = (named > 0) & (block_id // owned == me)

    def unit_copy(slot, local, way, target):
        return pltpu.make_async_remote_copy(
            src_ref=gath.at[slot],
            dst_ref=gath.at[slot],
            send_sem=send.at[local, way],
            recv_sem=recv.at[slot],
            device_id={"ctx": target},
            device_id_type=MESH,
        )

    def slot_of(zz, j):
        crossed = (j == units).astype(jnp.int32)
        yy = lax.rem(y + crossed, 2)
        u = j * (1 - crossed)
        return at(zz, yy, core) * units + u, (zz * 2 + yy) * units + u

    up = at(lax.rem(z + 1, line), y, core)
    down = at(lax.rem(z + line - 1, line), y, core)
    across = at(z, 1 - y, core)
    sibling = at(z, y, 1 - core)

    def sends(zz, j):
        valid = (zz >= 0) & (zz < line) & ((j < units) | (core == 1))
        own_line = j < units
        return (
            (0, up, valid & (zz <= z) & (z + 1 < line)),
            (1, down, valid & (zz >= z) & (z > 0)),
            (2, across, valid & own_line & ((zz == z) | (core == 0) | (j > 0))),
            (3, sibling, valid),
        )

    def forward(zz, j, skip=()):
        slot, local = slot_of(zz, j)
        for way, target, yes in sends(zz, j):
            if way not in skip:
                @pl.when(yes)
                def _():
                    unit_copy(slot, local, way, target).start()

    def arrived(slot):
        unit_copy(slot, 0, 0, sibling).wait_recv()

    past = ctx_count * owned
    fetch_cache.wait()
    last = jnp.int32(-1)
    token = lax.broadcasted_iota(jnp.int32, (pair, owned * BLOCK), 0)
    column = lax.broadcasted_iota(jnp.int32, (pair, owned * BLOCK), 1)
    for u in range(units):
        starts = []
        for h in range(2):
            last = jnp.min(jnp.where(mine & (block_id > last), block_id, past))
            starts.append(jnp.minimum(last - me * owned, owned - 1) * BLOCK)
        wanted = jnp.where(token < BLOCK, starts[0] + token, starts[1] + token - BLOCK)
        chosen = jnp.where(column == wanted, 1.0, 0.0).astype(jnp.bfloat16)
        tokens = lax.dot_general(
            chosen, near_cache[...], (((1,), (1,)), ((), ())), preferred_element_type=jnp.float32
        ).astype(jnp.bfloat16)
        tail = tokens[:, LAT:]
        packed = jnp.concatenate(
            [tail[i * tall : (i + 1) * tall, :] for i in range(pair // tall)], axis=1
        )
        gath[me * units + u, :pair, :] = tokens[:, :LAT]
        gath[me * units + u, pair:, :] = packed
        pool[me * units + u, :pair, :] = tokens[:, :LAT]
        pool[me * units + u, pair:, :] = packed
        forward(z, jnp.int32(u))

    def keep(slot):
        pool[slot] = gath[slot]

    fetch.wait()

    def turn(row):
        q_ref[row] = raw_q[row].T

    for k in range(TOPK):
        order[k] = jnp.sum(jnp.where(lane == k, ordered, 0))

    per = units + 1

    def along(k):
        step = k // per
        j = lax.rem(k, per)
        for zz in (z + 1 + step, z - 1 - step):
            @pl.when((zz >= 0) & (zz < line) & ((j < units) | (core == 1)))
            def _():
                slot, _ = slot_of(zz, j)
                arrived(slot)
                forward(zz, j)
                keep(slot)

    main = per * (line - 2)

    @pl.loop(0, main)
    def _(k):
        along(k)

        @pl.when((k == 0) & (core == 1))
        def _():
            slot, _ = slot_of(z, jnp.int32(units))
            arrived(slot)
            forward(z, jnp.int32(units))
            keep(slot)

        @pl.when(k < rows)
        def _():
            turn(lax.rem(k, rows))

    @pl.loop(min(rows, main), rows)
    def _(row):
        turn(row)

    def cross(zz, j):
        @pl.when((core == 0) | (j > 0))
        def _():
            slot = at(zz, 1 - y, core) * units + j
            local = (zz * 2 + 1 - y) * units + j
            arrived(slot)
            unit_copy(slot, local, 3, sibling).start()
            keep(slot)

    def beside(owner, u):
        slot = owner * units + u
        arrived(slot)
        keep(slot)

    @pl.loop(0, units * line)
    def _(k):
        zz = lax.rem(z + k // units, line)

        @pl.when(k // units == line - 2)
        def _():
            along(main + lax.rem(k, units))

        @pl.when(zz != far)
        def _():
            cross(zz, lax.rem(k, units))

    @pl.loop(0, line * 2 * units)
    def _(k):
        o = k // units

        @pl.when(o // 2 != far)
        def _():
            beside(o * 2 + 1 - core, lax.rem(k, units))

    def fill(first_block, blocks):
        for k in range(first_block, first_block + blocks, 2):
            latent, tails, places = [], [], []
            for h in range(2):
                p = order[k + h]
                owner = p // owned
                slot = jnp.sum(jnp.where((block_id // owned == owner) & (block_id < p), named, 0))
                unit = pool[owner * units + slot // 2]
                first = lax.rem(slot, 2) == 0
                latent.append(jnp.where(first, unit[:BLOCK], unit[BLOCK:pair]))
                tail = jnp.where(first, unit[pair:, : LAT // 2], unit[pair:, LAT // 2 :])
                tails += [tail[:, i * rope : (i + 1) * rope] for i in range(BLOCK // tall)]
                places.append(p * BLOCK)
            latent = jnp.concatenate(latent, axis=0)
            tails = jnp.concatenate(tails, axis=0)
            span = slice(k * BLOCK, (k + 2) * BLOCK)
            values[span, :] = latent
            keys_t[:LAT, span] = latent.T
            keys_t[LAT:, span] = tails.T
            positions[:, span] = jnp.where(lane < BLOCK, places[0] + lane, places[1] + lane - BLOCK)

    scale = SOFTMAX_SCALE * LOG2E
    merged = 2 if rows % 4 == 0 else 1
    groups = rows // 2 // merged

    def scores(i, span):
        q = q_ref[pl.ds(2 * i, 2)].reshape(2 * heads, feature)
        s = jnp.dot(q, keys_t[:, span], preferred_element_type=jnp.float32)
        where = positions[:, span]
        return jnp.concatenate(
            [
                jnp.where(where < lengths_ref[2 * i + r], s[r * heads : (r + 1) * heads], HIDDEN)
                for r in range(2)
            ],
            axis=0,
        )

    early = slice(0, early_blocks * BLOCK)
    late = slice(early_blocks * BLOCK, TOPK * BLOCK)
    fill(0, early_blocks)

    @pl.loop(0, groups)
    def _(g):
        for m in range(merged):
            i = g * merged + m
            s = scores(i, early)
            top = jnp.max(s, axis=1, keepdims=True)
            e = jnp.exp2((s - top) * scale)
            top_ref[i] = top
            total_ref[i] = jnp.sum(e, axis=1, keepdims=True)
            acc_ref[i] = jnp.dot(
                e.astype(jnp.bfloat16), values[early, :], preferred_element_type=jnp.float32
            )

        @pl.when(g < units)
        def _():
            cross(far, g)

    @pl.loop(min(units, groups), units)
    def _(u):
        cross(far, u)

    along(jnp.int32(main + units))

    @pl.loop(0, 2 * units)
    def _(k):
        beside(at(far, k // units, 1 - core), lax.rem(k, units))

    fill(early_blocks, late_blocks)

    @pl.loop(0, groups)
    def _(g):
        for m in range(merged):
            i = g * merged + m
            s = scores(i, late)
            before = top_ref[i]
            top = jnp.maximum(before, jnp.max(s, axis=1, keepdims=True))
            e = jnp.exp2((s - top) * scale)
            shrink = jnp.exp2((before - top) * scale)
            total = total_ref[i] * shrink + jnp.sum(e, axis=1, keepdims=True)
            o = acc_ref[i] * shrink + jnp.dot(
                e.astype(jnp.bfloat16), values[late, :], preferred_element_type=jnp.float32
            )
            out_ref[pl.ds(2 * i, 2)] = (o / total).astype(jnp.bfloat16).reshape(2, heads, LAT)

    @pl.loop(1, ctx_count)
    def _(d):
        flag_copy(d).wait_send()

    @pl.loop(0, per * line)
    def _(k):
        zz = k // per
        j = lax.rem(k, per)
        slot, local = slot_of(zz, j)
        for way, target, yes in sends(zz, j):
            @pl.when(yes)
            def _():
                unit_copy(slot, local, way, target).wait_send()

    @pl.loop(0, units * line)
    def _(k):
        zz = k // units
        j = lax.rem(k, units)

        @pl.when((core == 0) | (j > 0))
        def _():
            slot = at(zz, 1 - y, core) * units + j
            local = (zz * 2 + 1 - y) * units + j
            unit_copy(slot, local, 3, sibling).wait_send()


def shards(queries, latent_cache, block_picks, lengths):
    ctx_count = lax.axis_size("ctx")
    rows, heads, feature = queries.shape
    owned = latent_cache.shape[0] // BLOCK
    units = max(1, 2 * TOPK // ctx_count)
    flag_rows = -(-(ctx_count * owned) // LANES // 8) * 8
    tall = 2 * BLOCK + 2 * BLOCK * (feature - LAT) // LAT
    keys = TOPK * BLOCK
    return pl.pallas_call(
        functools.partial(step_kernel, ctx_count, owned, units),
        out_shape=pltpu.VMEM((rows, heads, LAT), jnp.bfloat16),
        in_specs=[
            pl.BlockSpec(memory_space=pltpu.SMEM),
            pl.BlockSpec(memory_space=pltpu.SMEM),
            pl.BlockSpec(memory_space=pl.ANY),
            pl.BlockSpec(memory_space=pl.ANY),
        ],
        out_specs=pl.BlockSpec(memory_space=pltpu.VMEM),
        scratch_shapes=[
            pltpu.VMEM((rows, feature, heads), jnp.bfloat16),
            pltpu.VMEM((feature, owned * BLOCK), jnp.bfloat16),
            pltpu.VMEM((rows, heads, feature), jnp.bfloat16),
            pltpu.VMEM((flag_rows, LANES), jnp.int32),
            pltpu.VMEM((ctx_count, flag_rows, LANES), jnp.int32),
            pltpu.VMEM((ctx_count * units, tall, LAT), jnp.bfloat16),
            pltpu.VMEM((ctx_count * units, tall, LAT), jnp.bfloat16),
            pltpu.VMEM((feature, keys), jnp.bfloat16),
            pltpu.VMEM((keys, LAT), jnp.bfloat16),
            pltpu.VMEM((1, keys), jnp.int32),
            pltpu.SMEM((TOPK,), jnp.int32),
            pltpu.VMEM((rows // 2, 2 * heads, 1), jnp.float32),
            pltpu.VMEM((rows // 2, 2 * heads, 1), jnp.float32),
            pltpu.VMEM((rows // 2, 2 * heads, LAT), jnp.float32),
            pltpu.SemaphoreType.DMA,
            pltpu.SemaphoreType.DMA,
            pltpu.SemaphoreType.DMA((ctx_count,)),
            pltpu.SemaphoreType.DMA((ctx_count,)),
            pltpu.SemaphoreType.DMA((ctx_count // 2 * units, 4)),
            pltpu.SemaphoreType.DMA((ctx_count * units,)),
        ],
        compiler_params=pltpu.CompilerParams(
            collective_id=0, has_side_effects=True, vmem_limit_bytes=64_900_000
        ),
    )(block_picks, lengths, jnp.swapaxes(queries, 1, 2), latent_cache.T)


def solution(mesh):
    placed = (
        P(("groups", "ctx"), None, None),
        P(("groups", "ctx"), None),
        P(("groups", "ctx"), None),
        P(("groups", "ctx")),
    )
    return jax.shard_map(
        shards,
        mesh=mesh,
        in_specs=placed,
        out_specs=P(("groups", "ctx"), None, None),
        check_vma=False,
    )
```

```python
import functools

import jax
import jax.numpy as jnp
from jax import lax
from jax.experimental import pallas as pl
from jax.experimental.pallas import tpu as pltpu
from jax.sharding import PartitionSpec as P

LAT = 512
BLOCK = 64
TOPK = 32
LANES = 128

SOFTMAX_SCALE = 192.0 ** (-0.5)
LOG2E = 1.4426950408889634
MESH = pl.DeviceIdType.MESH
HIDDEN = -1e30
CHUNK = 4


def step_kernel(
    ctx_count, owned, units, picks_ref, lengths_ref, queries_ref, cache_ref, out_ref,
    raw_q, near_cache, q_ref, flags_ref, all_flags, gath, pool, tails, keys, positions, order, slots,
    top_ref, total_ref, acc_ref, s_a, s_b, p_a, p_b, h_a, h_b,
    q_sem, cache_sem, flag_send, flag_recv, send, recv,
):
    rows, feature, heads = queries_ref.shape
    rope = feature - LAT
    pair = 2 * BLOCK
    tall = pair * rope // LAT
    line = ctx_count // 4
    span = max(1, units // 2)
    crossing = span if units > 1 else 0
    me = lax.axis_index("ctx")
    core = lax.rem(me, 2)
    y = lax.rem(me // 2, 2)
    z = me // 4

    fetch = pltpu.make_async_copy(queries_ref, raw_q, q_sem)
    fetch_cache = pltpu.make_async_copy(cache_ref, near_cache, cache_sem)
    fetch_cache.start()
    fetch.start()

    def at(zz, yy, cc):
        return (zz * 2 + yy) * 2 + cc

    barrier = pltpu.get_barrier_semaphore()

    @pl.loop(1, ctx_count)
    def _(d):
        pl.semaphore_signal(
            barrier, inc=1, device_id={"ctx": lax.rem(me + d, ctx_count)}, device_id_type=MESH
        )

    flag_rows = flags_ref.shape[0]
    block_id = lax.broadcasted_iota(jnp.int32, (flag_rows, LANES), 0) * LANES
    block_id += lax.broadcasted_iota(jnp.int32, (flag_rows, LANES), 1)
    lane = lax.broadcasted_iota(jnp.int32, (1, LANES), 1)
    flags = jnp.zeros((flag_rows, LANES), jnp.int32)
    for k in range(TOPK):
        flags = jnp.where(block_id == picks_ref[0, k], 1, flags)
    flags_ref[...] = flags

    pl.semaphore_wait(barrier, ctx_count - 1)

    def flag_copy(d):
        return pltpu.make_async_remote_copy(
            src_ref=flags_ref,
            dst_ref=all_flags.at[me],
            send_sem=flag_send.at[d],
            recv_sem=flag_recv.at[me],
            device_id={"ctx": lax.rem(me + d, ctx_count)},
            device_id_type=MESH,
        )

    def flag_arrival(source):
        return pltpu.make_async_remote_copy(
            src_ref=flags_ref,
            dst_ref=all_flags.at[source],
            send_sem=flag_send.at[0],
            recv_sem=flag_recv.at[source],
            device_id={"ctx": source},
            device_id_type=MESH,
        )

    @pl.loop(1, ctx_count)
    def _(d):
        flag_copy(d).start()

    all_flags[me] = flags

    def stage(p):
        owner = p // owned
        away = jnp.abs(owner // 4 - z)
        aside = (lax.rem(owner // 2, 2) != y).astype(jnp.int32)
        c = lax.rem(owner, 2)
        last = 3 + 2 * c + aside
        return jnp.where(away == line - 1, last, jnp.where(away == line - 2, aside * (1 + c), 0))

    stages = [stage(picks_ref[0, k]) for k in range(TOPK)]
    begin, total = [], jnp.int32(0)
    for v in range(7):
        begin.append(total)
        for k in range(TOPK):
            total += (stages[k] == v).astype(jnp.int32)
    ordered = jnp.zeros((1, LANES), jnp.int32)
    for k in range(TOPK):
        place = jnp.int32(0)
        for v in range(7):
            here = (stages[k] == v).astype(jnp.int32)
            place += here * begin[v]
            begin[v] += here
        ordered = jnp.where(lane == place, picks_ref[0, k], ordered)

    @pl.loop(1, ctx_count)
    def _(d):
        flag_arrival(lax.rem(me + d, ctx_count)).wait_recv()

    named = jnp.minimum(jnp.max(all_flags[...], axis=0), 1)
    mine = (named > 0) & (block_id // owned == me)

    def unit_copy(slot, local, way, target):
        return pltpu.make_async_remote_copy(
            src_ref=gath.at[slot],
            dst_ref=gath.at[slot],
            send_sem=send.at[local, way],
            recv_sem=recv.at[slot],
            device_id={"ctx": target},
            device_id_type=MESH,
        )

    def item(path, i):
        if units > 1:
            return i // span, path * span + lax.rem(i, span)
        return path, i * 0

    def slot_of(zz, j):
        crossed = (j == units).astype(jnp.int32)
        i = jnp.where(j == units, crossing, j)
        yy = lax.rem(y + crossed, 2)
        c, u = item(core, i)
        return at(zz, yy, c) * units + u, (zz * 2 + yy) * units + i, c

    up = at(lax.rem(z + 1, line), y, core)
    down = at(lax.rem(z + line - 1, line), y, core)
    across = at(z, 1 - y, core)
    sibling = at(z, y, 1 - core)

    def sends(zz, j, c):
        valid = (zz >= 0) & (zz < line) & ((j < units) | (core == 1))
        own_line = j < units
        return (
            (0, up, valid & (zz <= z) & (z + 1 < line)),
            (1, down, valid & (zz >= z) & (z > 0)),
            (2, across, valid & own_line & ((zz == z) | (core == 0) | (j != crossing))),
            (3, sibling, valid & ((zz != z) | (j == units) | (c == core))),
        )

    def forward(zz, j, skip=()):
        slot, local, c = slot_of(zz, j)
        for way, target, yes in sends(zz, j, c):
            if way not in skip:
                @pl.when(yes)
                def _():
                    unit_copy(slot, local, way, target).start()

    def arrived(slot):
        unit_copy(slot, 0, 0, sibling).wait_recv()

    def keep(slot):
        pool[2 * slot] = gath[slot, :BLOCK]
        pool[2 * slot + 1] = gath[slot, BLOCK:pair]
        tails[slot] = gath[slot, pair:]

    past = ctx_count * owned
    fetch_cache.wait()
    token = lax.broadcasted_iota(jnp.int32, (pair, owned * BLOCK), 0)
    column = lax.broadcasted_iota(jnp.int32, (pair, owned * BLOCK), 1)
    starts = []
    last = jnp.int32(-1)
    for _ in range(2 * units):
        last = jnp.min(jnp.where(mine & (block_id > last), block_id, past))
        starts.append(jnp.minimum(last - me * owned, owned - 1) * BLOCK)

    def other_path(u):
        return (z * 2 + y) * units + (1 - core) * span + u % span

    for u in [v for r in range(span) for v in range(r, units, span)]:
        first, second = starts[2 * u], starts[2 * u + 1]
        wanted = jnp.where(token < BLOCK, first + token, second + token - BLOCK)
        chosen = jnp.where(column == wanted, 1.0, 0.0).astype(jnp.bfloat16)
        tokens = lax.dot_general(
            chosen, near_cache[...], (((1,), (1,)), ((), ())), preferred_element_type=jnp.float32
        ).astype(jnp.bfloat16)
        tail = tokens[:, LAT:]
        packed = jnp.concatenate(
            [tail[i * tall : (i + 1) * tall, :] for i in range(pair // tall)], axis=1
        )
        gath[me * units + u, :pair, :] = tokens[:, :LAT]
        gath[me * units + u, pair:, :] = packed
        pool[2 * (me * units + u)] = tokens[:BLOCK, :LAT]
        pool[2 * (me * units + u) + 1] = tokens[BLOCK:, :LAT]
        tails[me * units + u] = packed
        if units == 1:
            forward(z, jnp.int32(0))
        else:
            path = u // span
            position = jnp.int32(path * span + u % span)

            @pl.when((core == path) & (core == 0))
            def _():
                forward(z, position)

            @pl.when((core == path) & (core == 1))
            def _():
                forward(z, position, (0, 1, 2))

            @pl.when(core != path)
            def _():
                unit_copy(me * units + u, other_path(u), 3, sibling).start()

    if units > 1:
        @pl.loop(0, units)
        def _(i):
            slot, _, c = slot_of(z, i)

            @pl.when(c != core)
            def _():
                arrived(slot)
                forward(z, i)
                keep(slot)

            @pl.when((c == core) & (core == 1))
            def _():
                forward(z, i, (3,))

    fetch.wait()

    for k in range(TOPK):
        p = jnp.sum(jnp.where(lane == k, ordered, 0))
        order[k] = p
        below = (block_id // owned == p // owned) & (block_id < p)
        slots[k] = jnp.sum(jnp.where(below, named, 0))

    def sides(d):
        return ((z + d, d >= 0), (z - d, d > 0))

    def along(d, j):
        for zz, yes in sides(d):
            @pl.when(yes & (zz >= 0) & (zz < line) & ((j < units) | (core == 1)))
            def _():
                slot, _, _ = slot_of(zz, j)
                arrived(slot)
                forward(zz, j)
                keep(slot)

    def cross(d, i):
        for zz, yes in sides(d):
            @pl.when(yes & (zz >= 0) & (zz < line) & ((core == 0) | (i != crossing)))
            def _():
                c, u = item(core, i)
                slot = at(zz, 1 - y, c) * units + u
                arrived(slot)
                unit_copy(slot, (zz * 2 + 1 - y) * units + i, 3, sibling).start()
                keep(slot)

    def beside(d, aside, i):
        c, u = item(1 - core, i)
        for zz, yes in sides(d):
            there = yes & (zz >= 0) & (zz < line)
            if not aside:
                there &= (d > 0) | (c != core)

            @pl.when(there)
            def _():
                yy = 1 - y if aside else y
                slot = at(zz, yy, c) * units + u
                arrived(slot)
                keep(slot)

    def each(c, path, body, lo=0, hi=None):
        if units > 1:
            pl.loop(c * span + lo, c * span + (span if hi is None else hi))(body)
        elif lo == 0:
            pl.when(path == c)(lambda: body(jnp.int32(0)))

    def cross_owner(d, c, lo=0, hi=None):
        each(c, core, lambda i: cross(jnp.int32(d), i), lo, hi)

    def along_owner(d, c, lo=0, hi=None):
        each(c, core, lambda i: along(jnp.int32(d), i), lo, hi)

    def beside_owner(d, aside, c):
        each(c, 1 - core, lambda i: beside(jnp.int32(d), aside, i))

    per = units + 1
    main = per * (line - 2)
    share = -(-rows // main)

    @pl.loop(0, main)
    def _(k):
        d = k // per + 1
        j = lax.rem(k, per)
        along(d, j)

        @pl.when((k == span) & (core == 1))
        def _():
            slot, _, _ = slot_of(z, jnp.int32(units))
            arrived(slot)
            forward(z, jnp.int32(units))
            keep(slot)

        @pl.when(j < units)
        def _():
            cross(d - 1, j)
            beside(d - 1, False, j)

        @pl.when((j < units) & (d > 1))
        def _():
            beside(d - 2, True, j)

        for r in range(share):
            @pl.when(k * share + r < rows)
            def _():
                row = lax.rem(k * share + r, rows)
                q_ref[row] = raw_q[row].T
                total_ref[pl.ds(row * heads, heads)] = jnp.zeros((heads, 1), jnp.float32)
                top_ref[pl.ds(row * heads, heads)] = jnp.full((heads, 1), HIDDEN, jnp.float32)
                acc_ref[pl.ds(row * heads, heads)] = jnp.zeros((heads, LAT), jnp.float32)

    @pl.loop(0, units)
    def _(i):
        beside(jnp.int32(line - 2), False, i)
        beside(jnp.int32(line - 3), True, i)

    scale = SOFTMAX_SCALE * LOG2E
    deep = CHUNK * BLOCK
    rowset = 4 if rows % 4 == 0 else 1
    groups = rows // rowset
    height = rowset * heads
    parts = 2 if rowset % 2 == 0 else 1

    def fill(n):
        places = []
        for k in range(CHUNK):
            p, slot = order[n * CHUNK + k], slots[n * CHUNK + k]
            here = slice(k * BLOCK, (k + 1) * BLOCK)
            keys[here, :LAT] = pool[p // owned * (2 * units) + slot]
            both = tails[p // owned * units + slot // 2]
            tail = jnp.where(lax.rem(slot, 2) == 0, both[:, : LAT // 2], both[:, LAT // 2 :])
            keys[here, LAT:] = jnp.concatenate(
                [tail[:, i * rope : (i + 1) * rope] for i in range(BLOCK // tall)], axis=0
            )
            places.append(p * BLOCK)
        for k in range(0, CHUNK, 2):
            positions[:, k * BLOCK : (k + 2) * BLOCK] = jnp.where(
                lane < BLOCK, places[k] + lane, places[k + 1] + lane - BLOCK
            )

    def qk(g, s_ref):
        for t in range(parts):
            low, many = g * rowset + t * rowset // parts, rowset // parts
            s_ref[t * height // parts : (t + 1) * height // parts] = lax.dot_general(
                q_ref[low : low + many].reshape(many * heads, feature), keys[...],
                (((1,), (1,)), ((), ())), preferred_element_type=jnp.float32,
            )

    def soft(g, s_ref, p_ref, h_ref):
        span_g = slice(g * height, (g + 1) * height)
        where = positions[...]
        s = jnp.concatenate(
            [
                jnp.where(
                    where < lengths_ref[g * rowset + r], s_ref[r * heads : (r + 1) * heads], HIDDEN
                )
                for r in range(rowset)
            ],
            axis=0,
        )
        before = top_ref[span_g]
        top = jnp.maximum(before, jnp.max(s, axis=1, keepdims=True))
        e = jnp.exp2((s - top) * scale)
        shrink = jnp.exp2((before - top) * scale)
        total_ref[span_g] = total_ref[span_g] * shrink + jnp.sum(e, axis=1, keepdims=True)
        top_ref[span_g] = top
        p_ref[...] = e.astype(jnp.bfloat16)
        h_ref[...] = shrink

    def pv(g, p_ref, h_ref, final):
        span_g = slice(g * height, (g + 1) * height)
        o = acc_ref[span_g] * h_ref[...] + jnp.dot(
            p_ref[...], keys[:, :LAT], preferred_element_type=jnp.float32
        )
        if final:
            o = (o / total_ref[span_g]).astype(jnp.bfloat16)
            out_ref[g * rowset : (g + 1) * rowset] = o.reshape(rowset, heads, LAT)
        else:
            acc_ref[span_g] = o

    def attend(n, final=False):
        fill(n)
        s, p, h = (s_a, s_b), (p_a, p_b), (h_a, h_b)
        for g in range(groups + 2):
            if g < groups:
                qk(g, s[g % 2])
            if 1 <= g <= groups:
                soft(g - 1, s[(g - 1) % 2], p[(g - 1) % 2], h[(g - 1) % 2])
            if g >= 2:
                pv(g - 2, p[g % 2], h[g % 2], final)

    ready = [(TOPK - (6 - v) * units) // CHUNK for v in range(7)]

    def attend_ready(v, lo=None, hi=None):
        lo = (ready[v - 1] if v else 0) if lo is None else lo
        hi = min(ready[v], TOPK // CHUNK - 1) if hi is None else hi
        if hi - lo == 1:
            attend(lo)
        elif hi > lo:
            pl.loop(lo, hi)(lambda n: attend(n))

    attend_ready(0, hi=1)
    cross_owner(line - 2, 0)
    attend_ready(0, lo=1)
    along_owner(line - 1, 0, 0, 1)
    beside_owner(line - 2, True, 0)
    attend_ready(1)
    cross_owner(line - 2, 1)
    along_owner(line - 1, 0, 1)
    beside_owner(line - 2, True, 1)
    attend_ready(2)
    along_owner(line - 1, 1, 0, 1)
    cross_owner(line - 1, 0, 0, 1)
    beside_owner(line - 1, False, 0)
    attend_ready(3)
    cross_owner(line - 1, 0, 1)
    along_owner(line - 1, 1, 1)
    beside_owner(line - 1, True, 0)
    attend_ready(4)
    along(jnp.int32(line - 1), jnp.int32(units))
    cross_owner(line - 1, 1, 0, 1)
    beside_owner(line - 1, False, 1)
    attend_ready(5)
    cross_owner(line - 1, 1, 1)
    beside_owner(line - 1, True, 1)
    attend(TOPK // CHUNK - 1, final=True)

    @pl.loop(1, ctx_count)
    def _(d):
        flag_copy(d).wait_send()

    @pl.loop(0, per * line)
    def _(k):
        zz = k // per
        j = lax.rem(k, per)
        slot, local, c = slot_of(zz, j)
        for way, target, yes in sends(zz, j, c):
            @pl.when(yes)
            def _():
                unit_copy(slot, local, way, target).wait_send()

    @pl.loop(0, units * line)
    def _(k):
        zz = k // units
        i = lax.rem(k, units)

        @pl.when((core == 0) | (i != crossing))
        def _():
            c, u = item(core, i)
            slot = at(zz, 1 - y, c) * units + u
            unit_copy(slot, (zz * 2 + 1 - y) * units + i, 3, sibling).wait_send()

    if units > 1:
        for u in range(units):
            @pl.when(core != u // span)
            def _():
                unit_copy(me * units + u, other_path(u), 3, sibling).wait_send()


def shards(queries, latent_cache, block_picks, lengths):
    ctx_count = lax.axis_size("ctx")
    rows, heads, feature = queries.shape
    owned = latent_cache.shape[0] // BLOCK
    units = max(1, 2 * TOPK // ctx_count)
    flag_rows = -(-(ctx_count * owned) // LANES // 8) * 8
    tall = 2 * BLOCK + 2 * BLOCK * (feature - LAT) // LAT
    height = (4 if rows % 4 == 0 else 1) * heads
    return pl.pallas_call(
        functools.partial(step_kernel, ctx_count, owned, units),
        out_shape=pltpu.VMEM((rows, heads, LAT), jnp.bfloat16),
        in_specs=[
            pl.BlockSpec(memory_space=pltpu.SMEM),
            pl.BlockSpec(memory_space=pltpu.SMEM),
            pl.BlockSpec(memory_space=pl.ANY),
            pl.BlockSpec(memory_space=pl.ANY),
        ],
        out_specs=pl.BlockSpec(memory_space=pltpu.VMEM),
        scratch_shapes=[
            pltpu.VMEM((rows, feature, heads), jnp.bfloat16),
            pltpu.VMEM((feature, owned * BLOCK), jnp.bfloat16),
            pltpu.VMEM((rows, heads, feature), jnp.bfloat16),
            pltpu.VMEM((flag_rows, LANES), jnp.int32),
            pltpu.VMEM((ctx_count, flag_rows, LANES), jnp.int32),
            pltpu.VMEM((ctx_count * units, tall, LAT), jnp.bfloat16),
            pltpu.VMEM((ctx_count * units * 2, BLOCK, LAT), jnp.bfloat16),
            pltpu.VMEM((ctx_count * units, tall - 2 * BLOCK, LAT), jnp.bfloat16),
            pltpu.VMEM((CHUNK * BLOCK, feature), jnp.bfloat16),
            pltpu.VMEM((1, CHUNK * BLOCK), jnp.int32),
            pltpu.SMEM((TOPK,), jnp.int32),
            pltpu.SMEM((TOPK,), jnp.int32),
            pltpu.VMEM((rows * heads, 1), jnp.float32),
            pltpu.VMEM((rows * heads, 1), jnp.float32),
            pltpu.VMEM((rows * heads, LAT), jnp.float32),
            *[pltpu.VMEM((height, CHUNK * BLOCK), jnp.float32)] * 2,
            *[pltpu.VMEM((height, CHUNK * BLOCK), jnp.bfloat16)] * 2,
            *[pltpu.VMEM((height, 1), jnp.float32)] * 2,
            pltpu.SemaphoreType.DMA,
            pltpu.SemaphoreType.DMA,
            pltpu.SemaphoreType.DMA((ctx_count,)),
            pltpu.SemaphoreType.DMA((ctx_count,)),
            pltpu.SemaphoreType.DMA((ctx_count // 2 * units, 4)),
            pltpu.SemaphoreType.DMA((ctx_count * units,)),
        ],
        compiler_params=pltpu.CompilerParams(
            collective_id=0, has_side_effects=True, vmem_limit_bytes=64_900_000
        ),
    )(block_picks, lengths, jnp.swapaxes(queries, 1, 2), latent_cache.T)


def solution(mesh):
    placed = (
        P(("groups", "ctx"), None, None),
        P(("groups", "ctx"), None),
        P(("groups", "ctx"), None),
        P(("groups", "ctx")),
    )
    return jax.shard_map(
        shards,
        mesh=mesh,
        in_specs=placed,
        out_specs=P(("groups", "ctx"), None, None),
        check_vma=False,
    )
```

```python
import functools

import jax
import jax.numpy as jnp
from jax import lax
from jax.experimental import pallas as pl
from jax.experimental.pallas import tpu as pltpu
from jax.sharding import PartitionSpec as P

LAT = 512
BLOCK = 64
TOPK = 32
LANES = 128

SOFTMAX_SCALE = 192.0 ** (-0.5)
LOG2E = 1.4426950408889634
MESH = pl.DeviceIdType.MESH
HIDDEN = -1e30
CHUNK = 4

EDGE = (
    110, 500, 111, 201, 113, 600, 202, 211, 301, 302, 114, 112, 300, 401, 311, 600, 120, 310,
    121, 212, 210, 313, 203, 321, 213, 600, 122, 320, 410, 402, 411, 200, 412, 220, 303, 312,
    123, 400, 413, 600, 403, 700, 221, 232, 420, 130, 124, 222, 323, 322, 701, 223, 422, 421,
    131, 702, 331, 330, 132, 423, 230, 703, 332, 133, 231, 704, 431, 430, 333, 705, 134, 233,
    706, 432, 433, 707,
)
INNER = (
    600, 500, 301, 202, 112, 110, 111, 600, 114, 402, 210, 410, 212, 312, 303, 310, 203, 200,
    113, 600, 311, 313, 120, 400, 403, 302, 600, 201, 211, 121, 321, 401, 122, 300, 123, 320,
    700, 323, 124, 322, 213, 701, 413, 222, 411, 702, 412, 422, 703, 704, 220, 223, 221, 705,
    420, 421, 423, 706, 707,
)


def step_kernel(
    ctx_count, owned, units, picks_ref, lengths_ref, queries_ref, cache_ref, out_ref,
    raw_q, near_cache, q_ref, flags_ref, all_flags, gath, pool, tails, keys, positions, listed_v, listed,
    top_ref, total_ref, acc_ref, s_a, s_b, p_a, p_b, h_a, h_b,
    q_sem, cache_sem, list_sem, flag_send, flag_recv, send, recv,
):
    rows, feature, heads = queries_ref.shape
    rope = feature - LAT
    pair = 2 * BLOCK
    tall = pair * rope // LAT
    line = ctx_count // 4
    span = max(1, units // 2)
    crossing = span if units > 1 else 0
    me = lax.axis_index("ctx")
    core = lax.rem(me, 2)
    y = lax.rem(me // 2, 2)
    z = me // 4

    fetch = pltpu.make_async_copy(queries_ref, raw_q, q_sem)
    fetch_cache = pltpu.make_async_copy(cache_ref, near_cache, cache_sem)
    fetch_cache.start()
    fetch.start()

    def at(zz, yy, cc):
        return (zz * 2 + yy) * 2 + cc

    barrier = pltpu.get_barrier_semaphore()

    @pl.loop(1, ctx_count)
    def _(d):
        pl.semaphore_signal(
            barrier, inc=1, device_id={"ctx": lax.rem(me + d, ctx_count)}, device_id_type=MESH
        )

    flag_rows = flags_ref.shape[0]
    block_id = lax.broadcasted_iota(jnp.int32, (flag_rows, LANES), 0) * LANES
    block_id += lax.broadcasted_iota(jnp.int32, (flag_rows, LANES), 1)
    lane = lax.broadcasted_iota(jnp.int32, (1, LANES), 1)
    flags = jnp.zeros((flag_rows, LANES), jnp.int32)
    for k in range(TOPK):
        flags = jnp.where(block_id == picks_ref[0, k], 1, flags)
    flags_ref[...] = flags

    pl.semaphore_wait(barrier, ctx_count - 1)

    def flag_copy(d):
        return pltpu.make_async_remote_copy(
            src_ref=flags_ref,
            dst_ref=all_flags.at[me],
            send_sem=flag_send.at[d],
            recv_sem=flag_recv.at[me],
            device_id={"ctx": lax.rem(me + d, ctx_count)},
            device_id_type=MESH,
        )

    def flag_arrival(source):
        return pltpu.make_async_remote_copy(
            src_ref=flags_ref,
            dst_ref=all_flags.at[source],
            send_sem=flag_send.at[0],
            recv_sem=flag_recv.at[source],
            device_id={"ctx": source},
            device_id_type=MESH,
        )

    @pl.loop(1, ctx_count)
    def _(d):
        flag_copy(d).start()

    all_flags[me] = flags

    scripted = line == 4 and units == 4 and TOPK // CHUNK == 8
    edge = (z == 0) | (z == line - 1)

    def stage(p):
        owner = p // owned
        away = jnp.abs(owner // 4 - z)
        aside = (lax.rem(owner // 2, 2) != y).astype(jnp.int32)
        c = lax.rem(owner, 2)
        if scripted:
            near = jnp.where(aside == 1, 2 + c, c)
            outer = jnp.where(away == 3, 4 + 2 * c + aside, jnp.where(away == 2, near, 0))
            near = jnp.where(away == 1, aside * (2 + 2 * c), 0)
            return jnp.where(edge, outer, jnp.where(away == 2, aside * 6 + c, near))
        last = 3 + 2 * c + aside
        return jnp.where(away == line - 1, last, jnp.where(away == line - 2, aside * (1 + c), 0))

    stages = [stage(picks_ref[0, k]) for k in range(TOPK)]
    begin, total = [], jnp.int32(0)
    for v in range(8):
        begin.append(total)
        for k in range(TOPK):
            total += (stages[k] == v).astype(jnp.int32)
    ordered = jnp.zeros((1, LANES), jnp.int32)
    for k in range(TOPK):
        place = jnp.int32(0)
        for v in range(8):
            here = (stages[k] == v).astype(jnp.int32)
            place += here * begin[v]
            begin[v] += here
        ordered = jnp.where(lane == place, picks_ref[0, k], ordered)

    @pl.loop(1, ctx_count)
    def _(d):
        flag_arrival(lax.rem(me + d, ctx_count)).wait_recv()

    named = jnp.minimum(jnp.max(all_flags[...], axis=0), 1)
    mine = (named > 0) & (block_id // owned == me)

    def unit_copy(slot, local, way, target):
        return pltpu.make_async_remote_copy(
            src_ref=gath.at[slot],
            dst_ref=gath.at[slot],
            send_sem=send.at[local, way],
            recv_sem=recv.at[slot],
            device_id={"ctx": target},
            device_id_type=MESH,
        )

    def item(path, i):
        if units > 1:
            return i // span, path * span + lax.rem(i, span)
        return path, i * 0

    def detoured(zz):
        if units > 1:
            return (core == 1) | (zz == 0) | (zz == line - 1)
        return core == 1

    def plain(zz, i):
        return jnp.logical_not(detoured(zz)) | (i != crossing)

    def slot_of(zz, j):
        crossed = (j == units).astype(jnp.int32)
        i = jnp.where(j == units, crossing, j)
        yy = lax.rem(y + crossed, 2)
        c, u = item(core, i)
        return at(zz, yy, c) * units + u, (zz * 2 + yy) * units + i, c

    up = at(lax.rem(z + 1, line), y, core)
    down = at(lax.rem(z + line - 1, line), y, core)
    across = at(z, 1 - y, core)
    sibling = at(z, y, 1 - core)

    def sends(zz, j, c):
        valid = (zz >= 0) & (zz < line) & ((j < units) | detoured(zz))
        own_line = j < units
        return (
            (0, up, valid & (zz <= z) & (z + 1 < line)),
            (1, down, valid & (zz >= z) & (z > 0)),
            (2, across, valid & own_line & ((zz == z) | plain(zz, j))),
            (3, sibling, valid & ((zz != z) | (j == units) | (c == core))),
        )

    def forward(zz, j, skip=()):
        slot, local, c = slot_of(zz, j)
        for way, target, yes in sends(zz, j, c):
            if way not in skip:
                @pl.when(yes)
                def _():
                    unit_copy(slot, local, way, target).start()

    def arrived(slot):
        unit_copy(slot, 0, 0, sibling).wait_recv()

    def keep(slot):
        pool[2 * slot] = gath[slot, :BLOCK]
        pool[2 * slot + 1] = gath[slot, BLOCK:pair]
        tails[slot] = gath[slot, pair:]

    past = ctx_count * owned
    fetch_cache.wait()
    token = lax.broadcasted_iota(jnp.int32, (pair, owned * BLOCK), 0)
    column = lax.broadcasted_iota(jnp.int32, (pair, owned * BLOCK), 1)
    starts = []
    last = jnp.int32(-1)

    def other_path(u):
        return (z * 2 + y) * units + (1 - core) * span + u % span

    for u in [v for r in range(span) for v in range(r, units, span)]:
        while len(starts) < 2 * u + 2:
            last = jnp.min(jnp.where(mine & (block_id > last), block_id, past))
            starts.append(jnp.minimum(last - me * owned, owned - 1) * BLOCK)
        first, second = starts[2 * u], starts[2 * u + 1]
        wanted = jnp.where(token < BLOCK, first + token, second + token - BLOCK)
        chosen = jnp.where(column == wanted, 1.0, 0.0).astype(jnp.bfloat16)
        tokens = lax.dot_general(
            chosen, near_cache[...], (((1,), (1,)), ((), ())), preferred_element_type=jnp.float32
        ).astype(jnp.bfloat16)
        tail = tokens[:, LAT:]
        packed = jnp.concatenate(
            [tail[i * tall : (i + 1) * tall, :] for i in range(pair // tall)], axis=1
        )
        gath[me * units + u, :pair, :] = tokens[:, :LAT]
        gath[me * units + u, pair:, :] = packed
        pool[2 * (me * units + u)] = tokens[:BLOCK, :LAT]
        pool[2 * (me * units + u) + 1] = tokens[BLOCK:, :LAT]
        tails[me * units + u] = packed
        if units == 1:
            forward(z, jnp.int32(0))
        else:
            path = u // span
            position = jnp.int32(path * span + u % span)

            @pl.when((core == path) & (core == 0))
            def _():
                forward(z, position)

            @pl.when((core == path) & (core == 1))
            def _():
                forward(z, position, (0, 1, 2))

            @pl.when(core != path)
            def _():
                unit_copy(me * units + u, other_path(u), 3, sibling).start()

    if units > 1:
        @pl.loop(0, units)
        def _(i):
            slot, _, c = slot_of(z, i)

            @pl.when(c != core)
            def _():
                arrived(slot)
                forward(z, i)
                keep(slot)

            @pl.when((c == core) & (core == 1))
            def _():
                forward(z, i, (3,))

    fetch.wait()

    within = lax.rem(block_id, owned)
    before = named
    shift = 1
    while shift < owned:
        before += jnp.where(within >= shift, pltpu.roll(before, shift, 1), 0)
        shift *= 2
    before -= named
    wide = lax.broadcasted_iota(jnp.int32, (TOPK, LANES), 1)
    tall_id = lax.broadcasted_iota(jnp.int32, (TOPK, LANES), 0)
    column_p = jnp.sum(jnp.where(wide == tall_id, ordered, 0), axis=1, keepdims=True)
    found = jnp.zeros((TOPK, LANES), jnp.int32)
    for r in range(-(-past // LANES)):
        found += jnp.where(column_p == wide + r * LANES, before[r : r + 1, :], 0)
    column_s = jnp.sum(found, axis=1, keepdims=True)
    listed_v[...] = jnp.where(wide == 0, column_p, column_s)
    listing = pltpu.make_async_copy(listed_v, listed, list_sem)
    listing.start()

    def sides(d, inner=True):
        if not scripted:
            return ((z + d, d >= 0), (z - d, d > 0))
        if inner and d == 1:
            return ((z + 1, True), (z - 1, True))
        return ((jnp.where(z + d < line, z + d, z - d), True),)

    def along(d, j, inner=True):
        for zz, yes in sides(d, inner):
            @pl.when(yes & (zz >= 0) & (zz < line) & ((j < units) | detoured(zz)))
            def _():
                slot, _, _ = slot_of(zz, j)
                arrived(slot)
                forward(zz, j)
                keep(slot)

    def cross(d, i, inner=True):
        for zz, yes in sides(d, inner):
            @pl.when(yes & (zz >= 0) & (zz < line) & plain(zz, i))
            def _():
                c, u = item(core, i)
                slot = at(zz, 1 - y, c) * units + u
                arrived(slot)
                unit_copy(slot, (zz * 2 + 1 - y) * units + i, 3, sibling).start()
                keep(slot)

    def beside(d, aside, i, inner=True):
        c, u = item(1 - core, i)
        for zz, yes in sides(d, inner):
            there = yes & (zz >= 0) & (zz < line)
            if not aside:
                there &= (d > 0) | (c != core)

            @pl.when(there)
            def _():
                yy = 1 - y if aside else y
                slot = at(zz, yy, c) * units + u
                arrived(slot)
                keep(slot)

    def each(c, path, body, lo=0, hi=None):
        if units > 1:
            pl.loop(c * span + lo, c * span + (span if hi is None else hi))(body)
        elif lo == 0:
            pl.when(path == c)(lambda: body(jnp.int32(0)))

    def cross_owner(d, c, lo=0, hi=None):
        each(c, core, lambda i: cross(jnp.int32(d), i), lo, hi)

    def along_owner(d, c, lo=0, hi=None):
        each(c, core, lambda i: along(jnp.int32(d), i), lo, hi)

    def beside_owner(d, aside, c):
        each(c, 1 - core, lambda i: beside(jnp.int32(d), aside, i))

    per = units + 1

    def crossing_unit():
        @pl.when(detoured(z))
        def _():
            slot, _, _ = slot_of(z, jnp.int32(units))
            arrived(slot)
            forward(z, jnp.int32(units))
            keep(slot)

    def prepare(row):
        q_ref[row] = raw_q[row].T
        total_ref[pl.ds(row * heads, heads)] = jnp.zeros((heads, 1), jnp.float32)
        top_ref[pl.ds(row * heads, heads)] = jnp.full((heads, 1), HIDDEN, jnp.float32)
        acc_ref[pl.ds(row * heads, heads)] = jnp.zeros((heads, LAT), jnp.float32)

    scale = SOFTMAX_SCALE * LOG2E
    deep = CHUNK * BLOCK
    rowset = 4 if rows % 4 == 0 else 1
    groups = rows // rowset
    height = rowset * heads
    parts = 2 if rowset % 2 == 0 else 1

    def fill(n):
        places = []
        for k in range(CHUNK):
            p, slot = listed[n * CHUNK + k, 0], listed[n * CHUNK + k, 1]
            here = slice(k * BLOCK, (k + 1) * BLOCK)
            keys[here, :LAT] = pool[p // owned * (2 * units) + slot]
            both = tails[p // owned * units + slot // 2]
            tail = jnp.where(lax.rem(slot, 2) == 0, both[:, : LAT // 2], both[:, LAT // 2 :])
            keys[here, LAT:] = jnp.concatenate(
                [tail[:, i * rope : (i + 1) * rope] for i in range(BLOCK // tall)], axis=0
            )
            places.append(p * BLOCK)
        for k in range(0, CHUNK, 2):
            positions[:, k * BLOCK : (k + 2) * BLOCK] = jnp.where(
                lane < BLOCK, places[k] + lane, places[k + 1] + lane - BLOCK
            )

    def qk(g, s_ref):
        for t in range(parts):
            low, many = g * rowset + t * rowset // parts, rowset // parts
            s_ref[t * height // parts : (t + 1) * height // parts] = lax.dot_general(
                q_ref[low : low + many].reshape(many * heads, feature), keys[...],
                (((1,), (1,)), ((), ())), preferred_element_type=jnp.float32,
            )

    def soft(g, s_ref, p_ref, h_ref):
        span_g = slice(g * height, (g + 1) * height)
        where = positions[...]
        s = jnp.concatenate(
            [
                jnp.where(
                    where < lengths_ref[g * rowset + r], s_ref[r * heads : (r + 1) * heads], HIDDEN
                )
                for r in range(rowset)
            ],
            axis=0,
        )
        before = top_ref[span_g]
        top = jnp.maximum(before, jnp.max(s, axis=1, keepdims=True))
        e = jnp.exp2((s - top) * scale)
        shrink = jnp.exp2((before - top) * scale)
        total_ref[span_g] = total_ref[span_g] * shrink + jnp.sum(e, axis=1, keepdims=True)
        top_ref[span_g] = top
        p_ref[...] = e.astype(jnp.bfloat16)
        h_ref[...] = shrink

    def pv(g, p_ref, h_ref, final):
        span_g = slice(g * height, (g + 1) * height)
        o = acc_ref[span_g] * h_ref[...] + jnp.dot(
            p_ref[...], keys[:, :LAT], preferred_element_type=jnp.float32
        )
        if final:
            o = (o * (1.0 / total_ref[span_g])).astype(jnp.bfloat16)
            out_ref[g * rowset : (g + 1) * rowset] = o.reshape(rowset, heads, LAT)
        else:
            acc_ref[span_g] = o

    def attend(n, final=False):
        fill(n)
        s, p, h = (s_a, s_b), (p_a, p_b), (h_a, h_b)
        for g in range(groups + 2):
            if g < groups:
                qk(g, s[g % 2])
            if 1 <= g <= groups:
                soft(g - 1, s[(g - 1) % 2], p[(g - 1) % 2], h[(g - 1) % 2])
            if g >= 2:
                pv(g - 2, p[g % 2], h[g % 2], final)

    def generic():
        main = per * (line - 2)
        share = -(-rows // main)

        @pl.loop(0, main)
        def _(k):
            d = k // per + 1
            j = lax.rem(k, per)
            along(d, j)

            pl.when(k == span)(crossing_unit)

            @pl.when(j < units)
            def _():
                cross(d - 1, j)
                beside(d - 1, False, j)

            @pl.when((j < units) & (d > 1))
            def _():
                beside(d - 2, True, j)

            for r in range(share):
                @pl.when(k * share + r < rows)
                def _():
                    prepare(lax.rem(k * share + r, rows))

        @pl.loop(0, units)
        def _(i):
            beside(jnp.int32(line - 2), False, i)
            beside(jnp.int32(line - 3), True, i)

        ready = [(TOPK - (6 - v) * units) // CHUNK for v in range(7)]

        def attend_ready(v, lo=None, hi=None):
            lo = (ready[v - 1] if v else 0) if lo is None else lo
            hi = min(ready[v], TOPK // CHUNK - 1) if hi is None else hi
            if hi - lo == 1:
                attend(lo)
            elif hi > lo:
                pl.loop(lo, hi)(lambda n: attend(n))

        attend_ready(0, hi=1)
        cross_owner(line - 2, 0)
        attend_ready(0, lo=1)
        along_owner(line - 1, 0, 0, 1)
        beside_owner(line - 2, True, 0)
        attend_ready(1)
        cross_owner(line - 2, 1)
        along_owner(line - 1, 0, 1)
        beside_owner(line - 2, True, 1)
        attend_ready(2)
        along_owner(line - 1, 1, 0, 1)
        cross_owner(line - 1, 0, 0, 1)
        beside_owner(line - 1, False, 0)
        attend_ready(3)
        cross_owner(line - 1, 0, 1)
        along_owner(line - 1, 1, 1)
        beside_owner(line - 1, True, 0)
        attend_ready(4)
        along(jnp.int32(line - 1), jnp.int32(units))
        cross_owner(line - 1, 1, 0, 1)
        beside_owner(line - 1, False, 1)
        attend_ready(5)
        cross_owner(line - 1, 1, 1)
        beside_owner(line - 1, True, 1)
        attend(TOPK // CHUNK - 1, final=True)

    def perform(work, inner):
        for w in work:
            kind, d, i = w // 100, w // 10 % 10, jnp.int32(w % 10)
            if kind == 1:
                along(d, i, inner)
            elif kind == 2:
                cross(d, i, inner)
            elif kind in (3, 4):
                beside(d, kind == 4, i, inner)
            elif kind == 5:
                crossing_unit()

    def preparation(work, before):
        shares = EDGE.count(600)
        pl.loop(before * rows // shares, (before + work) * rows // shares)(prepare)

    def pieces(work, chunk):
        starts = [0] + [work.index(700 + n) + 1 for n in range(8)]
        return work[starts[chunk] : starts[chunk + 1] - 1]

    def emit(work, inner):
        done, batch = 0, []
        for w in work + (0,):
            if w in (0, 600):
                perform(batch, inner)
                batch = []
                if w:
                    preparation(1, done)
                    done += 1
            else:
                batch.append(w)

    listing.wait()
    if scripted:
        for n in range(8):
            pl.when(edge)(lambda: emit(pieces(EDGE, n), False))
            pl.when(jnp.logical_not(edge))(lambda: emit(pieces(INNER, n), True))
            attend(n, final=n == 7)
    else:
        generic()

    @pl.loop(1, ctx_count)
    def _(d):
        flag_copy(d).wait_send()

    @pl.loop(0, per * line)
    def _(k):
        zz = k // per
        j = lax.rem(k, per)
        slot, local, c = slot_of(zz, j)
        for way, target, yes in sends(zz, j, c):
            @pl.when(yes)
            def _():
                unit_copy(slot, local, way, target).wait_send()

    @pl.loop(0, units * line)
    def _(k):
        zz = k // units
        i = lax.rem(k, units)

        @pl.when(plain(zz, i))
        def _():
            c, u = item(core, i)
            slot = at(zz, 1 - y, c) * units + u
            unit_copy(slot, (zz * 2 + 1 - y) * units + i, 3, sibling).wait_send()

    if units > 1:
        for u in range(units):
            @pl.when(core != u // span)
            def _():
                unit_copy(me * units + u, other_path(u), 3, sibling).wait_send()


def shards(queries, latent_cache, block_picks, lengths):
    ctx_count = lax.axis_size("ctx")
    rows, heads, feature = queries.shape
    owned = latent_cache.shape[0] // BLOCK
    units = max(1, 2 * TOPK // ctx_count)
    flag_rows = -(-(ctx_count * owned) // LANES // 8) * 8
    tall = 2 * BLOCK + 2 * BLOCK * (feature - LAT) // LAT
    height = (4 if rows % 4 == 0 else 1) * heads
    return pl.pallas_call(
        functools.partial(step_kernel, ctx_count, owned, units),
        out_shape=pltpu.VMEM((rows, heads, LAT), jnp.bfloat16),
        in_specs=[
            pl.BlockSpec(memory_space=pltpu.SMEM),
            pl.BlockSpec(memory_space=pltpu.SMEM),
            pl.BlockSpec(memory_space=pl.ANY),
            pl.BlockSpec(memory_space=pl.ANY),
        ],
        out_specs=pl.BlockSpec(memory_space=pltpu.VMEM),
        scratch_shapes=[
            pltpu.VMEM((rows, feature, heads), jnp.bfloat16),
            pltpu.VMEM((feature, owned * BLOCK), jnp.bfloat16),
            pltpu.VMEM((rows, heads, feature), jnp.bfloat16),
            pltpu.VMEM((flag_rows, LANES), jnp.int32),
            pltpu.VMEM((ctx_count, flag_rows, LANES), jnp.int32),
            pltpu.VMEM((ctx_count * units, tall, LAT), jnp.bfloat16),
            pltpu.VMEM((ctx_count * units * 2, BLOCK, LAT), jnp.bfloat16),
            pltpu.VMEM((ctx_count * units, tall - 2 * BLOCK, LAT), jnp.bfloat16),
            pltpu.VMEM((CHUNK * BLOCK, feature), jnp.bfloat16),
            pltpu.VMEM((1, CHUNK * BLOCK), jnp.int32),
            pltpu.VMEM((TOPK, LANES), jnp.int32),
            pltpu.SMEM((TOPK, LANES), jnp.int32),
            pltpu.VMEM((rows * heads, 1), jnp.float32),
            pltpu.VMEM((rows * heads, 1), jnp.float32),
            pltpu.VMEM((rows * heads, LAT), jnp.float32),
            *[pltpu.VMEM((height, CHUNK * BLOCK), jnp.float32)] * 2,
            *[pltpu.VMEM((height, CHUNK * BLOCK), jnp.bfloat16)] * 2,
            *[pltpu.VMEM((height, 1), jnp.float32)] * 2,
            pltpu.SemaphoreType.DMA,
            pltpu.SemaphoreType.DMA,
            pltpu.SemaphoreType.DMA,
            pltpu.SemaphoreType.DMA((ctx_count,)),
            pltpu.SemaphoreType.DMA((ctx_count,)),
            pltpu.SemaphoreType.DMA((ctx_count // 2 * units, 4)),
            pltpu.SemaphoreType.DMA((ctx_count * units,)),
        ],
        compiler_params=pltpu.CompilerParams(
            collective_id=0, has_side_effects=True, vmem_limit_bytes=64_900_000
        ),
    )(block_picks, lengths, jnp.swapaxes(queries, 1, 2), latent_cache.T)


def solution(mesh):
    placed = (
        P(("groups", "ctx"), None, None),
        P(("groups", "ctx"), None),
        P(("groups", "ctx"), None),
        P(("groups", "ctx")),
    )
    return jax.shard_map(
        shards,
        mesh=mesh,
        in_specs=placed,
        out_specs=P(("groups", "ctx"), None, None),
        check_vma=False,
    )
```

```python
import functools

import jax
import jax.numpy as jnp
from jax import lax
from jax.experimental import pallas as pl
from jax.experimental.pallas import tpu as pltpu
from jax.sharding import PartitionSpec as P

LAT = 512
BLOCK = 64
TOPK = 32
LANES = 128

SOFTMAX_SCALE = 192.0 ** (-0.5)
LOG2E = 1.4426950408889634
MESH = pl.DeviceIdType.MESH
HIDDEN = -1e30
CHUNK = 4

EDGE = (
    111, 110, 300, 500, 112, 600, 311, 113, 310, 203, 120, 320, 302, 210, 201, 122, 313, 303,
    402, 312, 202, 211, 213, 121, 200, 411, 600, 413, 114, 403, 401, 123, 212, 600, 600, 301,
    321, 410, 400, 412, 222, 322, 220, 700, 124, 323, 420, 130, 232, 221, 701, 223, 131, 421,
    330, 422, 702, 423, 331, 230, 703, 133, 430, 231, 704, 132, 431, 705, 233, 333, 332, 134,
    706, 433, 432, 707,
)
INNER = (
    303, 110, 112, 111, 500, 210, 312, 113, 410, 600, 310, 114, 200, 202, 212, 120, 201, 302,
    402, 211, 600, 401, 203, 121, 320, 301, 600, 321, 123, 313, 300, 122, 403, 600, 311, 400,
    323, 411, 700, 322, 124, 213, 701, 412, 413, 702, 703, 223, 222, 422, 220, 221, 704, 421,
    420, 705, 423, 706, 707,
)


def step_kernel(
    ctx_count, owned, units, picks_hbm, lengths_hbm, queries_ref, cache_ref, out_ref,
    picks_ref, lengths_ref, raw_q, near_cache, near, near_tails, q_ref, flags_ref, all_flags, gath, pool, tails, keys, positions, listed_v, listed,
    top_ref, total_ref, acc_ref, s_a, s_b, p_a, p_b, h_a, h_b,
    picks_sem, lengths_sem, q_sem, cache_sem, list_sem, flag_send, flag_recv, send, recv,
):
    rows, feature, heads = queries_ref.shape
    rope = feature - LAT
    pair = 2 * BLOCK
    tall = pair * rope // LAT
    line = ctx_count // 4
    span = max(1, units // 2)
    crossing = span if units > 1 else 0
    me = lax.axis_index("ctx")
    core = lax.rem(me, 2)
    y = lax.rem(me // 2, 2)
    z = me // 4

    fetch = pltpu.make_async_copy(queries_ref, raw_q, q_sem)
    fetch_cache = pltpu.make_async_copy(cache_ref, near_cache, cache_sem)
    fetch_picks = pltpu.make_async_copy(picks_hbm, picks_ref, picks_sem)
    fetch_lengths = pltpu.make_async_copy(lengths_hbm, lengths_ref, lengths_sem)
    fetch_picks.start()

    def at(zz, yy, cc):
        return (zz * 2 + yy) * 2 + cc

    barrier = pltpu.get_barrier_semaphore()

    @pl.loop(1, ctx_count)
    def _(d):
        pl.semaphore_signal(
            barrier, inc=1, device_id={"ctx": lax.rem(me + d, ctx_count)}, device_id_type=MESH
        )

    fetch_cache.start()
    fetch_lengths.start()
    fetch.start()
    fetch_picks.wait()
    flag_rows = flags_ref.shape[0]
    block_id = lax.broadcasted_iota(jnp.int32, (flag_rows, LANES), 0) * LANES
    block_id += lax.broadcasted_iota(jnp.int32, (flag_rows, LANES), 1)
    lane = lax.broadcasted_iota(jnp.int32, (1, LANES), 1)
    flags = jnp.zeros((flag_rows, LANES), jnp.int32)
    for k in range(TOPK):
        flags = jnp.where(block_id == picks_ref[0, k], 1, flags)
    flags_ref[...] = flags

    pl.semaphore_wait(barrier, ctx_count - 1)

    def flag_copy(d):
        return pltpu.make_async_remote_copy(
            src_ref=flags_ref,
            dst_ref=all_flags.at[me],
            send_sem=flag_send.at[d],
            recv_sem=flag_recv.at[me],
            device_id={"ctx": lax.rem(me + d, ctx_count)},
            device_id_type=MESH,
        )

    def flag_arrival(source):
        return pltpu.make_async_remote_copy(
            src_ref=flags_ref,
            dst_ref=all_flags.at[source],
            send_sem=flag_send.at[0],
            recv_sem=flag_recv.at[source],
            device_id={"ctx": source},
            device_id_type=MESH,
        )

    @pl.loop(1, ctx_count)
    def _(d):
        flag_copy(d).start()

    all_flags[me] = flags

    scripted = line == 4 and units == 4 and TOPK // CHUNK == 8
    edge = (z == 0) | (z == line - 1)

    def stage(p):
        owner = p // owned
        away = jnp.abs(owner // 4 - z)
        aside = (lax.rem(owner // 2, 2) != y).astype(jnp.int32)
        c = lax.rem(owner, 2)
        if scripted:
            near = jnp.where(aside == 1, 2 + c, c)
            outer = jnp.where(away == 3, 4 + 2 * c + aside, jnp.where(away == 2, near, 0))
            near = jnp.where(away == 1, aside * (2 + 2 * c), 0)
            return jnp.where(edge, outer, jnp.where(away == 2, aside * 6 + c, near))
        last = 3 + 2 * c + aside
        return jnp.where(away == line - 1, last, jnp.where(away == line - 2, aside * (1 + c), 0))

    stages = [stage(picks_ref[0, k]) for k in range(TOPK)]
    begin, total = [], jnp.int32(0)
    for v in range(8):
        begin.append(total)
        for k in range(TOPK):
            total += (stages[k] == v).astype(jnp.int32)
    ordered = jnp.zeros((1, LANES), jnp.int32)
    for k in range(TOPK):
        place = jnp.int32(0)
        for v in range(8):
            here = (stages[k] == v).astype(jnp.int32)
            place += here * begin[v]
            begin[v] += here
        ordered = jnp.where(lane == place, picks_ref[0, k], ordered)

    fetch_cache.wait()

    @pl.loop(0, owned // 2)
    def _(b):
        tokens = near_cache[:, pl.ds(pl.multiple_of(b * pair, pair), pair)].T
        tail = tokens[:, LAT:]
        packed = jnp.concatenate(
            [tail[i * tall : (i + 1) * tall, :] for i in range(pair // tall)], axis=1
        )
        near[2 * b] = tokens[:BLOCK, :LAT]
        near[2 * b + 1] = tokens[BLOCK:, :LAT]
        near_tails[2 * b] = packed[:, : LAT // 2]
        near_tails[2 * b + 1] = packed[:, LAT // 2 :]

    @pl.loop(1, ctx_count)
    def _(d):
        flag_arrival(lax.rem(me + d, ctx_count)).wait_recv()

    named = jnp.minimum(jnp.max(all_flags[...], axis=0), 1)
    mine = (named > 0) & (block_id // owned == me)

    def unit_copy(slot, local, way, target):
        return pltpu.make_async_remote_copy(
            src_ref=gath.at[slot],
            dst_ref=gath.at[slot],
            send_sem=send.at[local, way],
            recv_sem=recv.at[slot],
            device_id={"ctx": target},
            device_id_type=MESH,
        )

    def item(path, i):
        if units > 1:
            return i // span, path * span + lax.rem(i, span)
        return path, i * 0

    def detoured(zz):
        if units > 1:
            return (core == 1) | (zz == 0) | (zz == line - 1)
        return core == 1

    def plain(zz, i):
        return jnp.logical_not(detoured(zz)) | (i != crossing)

    def slot_of(zz, j):
        crossed = (j == units).astype(jnp.int32)
        i = jnp.where(j == units, crossing, j)
        yy = lax.rem(y + crossed, 2)
        c, u = item(core, i)
        return at(zz, yy, c) * units + u, (zz * 2 + yy) * units + i, c

    up = at(lax.rem(z + 1, line), y, core)
    down = at(lax.rem(z + line - 1, line), y, core)
    across = at(z, 1 - y, core)
    sibling = at(z, y, 1 - core)

    def sends(zz, j, c):
        valid = (zz >= 0) & (zz < line) & ((j < units) | detoured(zz))
        own_line = j < units
        return (
            (0, up, valid & (zz <= z) & (z + 1 < line)),
            (1, down, valid & (zz >= z) & (z > 0)),
            (2, across, valid & own_line & ((zz == z) | plain(zz, j))),
            (3, sibling, valid & ((zz != z) | (j == units) | (c == core))),
        )

    def forward(zz, j, skip=()):
        slot, local, c = slot_of(zz, j)
        for way, target, yes in sends(zz, j, c):
            if way not in skip:
                @pl.when(yes)
                def _():
                    unit_copy(slot, local, way, target).start()

    def arrived(slot):
        unit_copy(slot, 0, 0, sibling).wait_recv()

    def keep(slot):
        pool[2 * slot] = gath[slot, :BLOCK]
        pool[2 * slot + 1] = gath[slot, BLOCK:pair]
        tails[slot] = gath[slot, pair:]

    past = ctx_count * owned
    starts = []
    last = jnp.int32(-1)

    def other_path(u):
        return (z * 2 + y) * units + (1 - core) * span + u % span

    for u in [v for r in range(span) for v in range(r, units, span)]:
        while len(starts) < 2 * u + 2:
            last = jnp.min(jnp.where(mine & (block_id > last), block_id, past))
            starts.append(jnp.minimum(last - me * owned, owned - 1))
        unit = me * units + u
        for h in range(2):
            block = starts[2 * u + h]
            gath[unit, h * BLOCK : (h + 1) * BLOCK, :] = near[block]
            gath[unit, pair:, h * LAT // 2 : (h + 1) * LAT // 2] = near_tails[block]
        if units == 1:
            forward(z, jnp.int32(0))
        else:
            path = u // span
            position = jnp.int32(path * span + u % span)

            @pl.when((core == path) & (core == 0))
            def _():
                forward(z, position)

            @pl.when((core == path) & (core == 1))
            def _():
                forward(z, position, (0, 1, 2))

            @pl.when(core != path)
            def _():
                unit_copy(me * units + u, other_path(u), 3, sibling).start()

    @pl.loop(0, units)
    def _(u):
        keep(me * units + u)

    if units > 1:
        @pl.loop(0, units)
        def _(i):
            slot, _, c = slot_of(z, i)

            @pl.when(c != core)
            def _():
                arrived(slot)
                forward(z, i)
                keep(slot)

            @pl.when((c == core) & (core == 1))
            def _():
                forward(z, i, (3,))

    fetch.wait()

    within = lax.rem(block_id, owned)
    before = named
    shift = 1
    while shift < owned:
        before += jnp.where(within >= shift, pltpu.roll(before, shift, 1), 0)
        shift *= 2
    before -= named
    wide = lax.broadcasted_iota(jnp.int32, (TOPK, LANES), 1)
    tall_id = lax.broadcasted_iota(jnp.int32, (TOPK, LANES), 0)
    column_p = jnp.sum(jnp.where(wide == tall_id, ordered, 0), axis=1, keepdims=True)
    found = jnp.zeros((TOPK, LANES), jnp.int32)
    for r in range(-(-past // LANES)):
        found += jnp.where(column_p == wide + r * LANES, before[r : r + 1, :], 0)
    column_s = jnp.sum(found, axis=1, keepdims=True)
    listed_v[...] = jnp.where(wide == 0, column_p, column_s)
    listing = pltpu.make_async_copy(listed_v, listed, list_sem)
    listing.start()

    def sides(d, inner=True):
        if not scripted:
            return ((z + d, d >= 0), (z - d, d > 0))
        if inner and d == 1:
            return ((z + 1, True), (z - 1, True))
        return ((jnp.where(z + d < line, z + d, z - d), True),)

    def along(d, j, inner=True):
        for zz, yes in sides(d, inner):
            @pl.when(yes & (zz >= 0) & (zz < line) & ((j < units) | detoured(zz)))
            def _():
                slot, _, _ = slot_of(zz, j)
                arrived(slot)
                forward(zz, j)
                keep(slot)

    def cross(d, i, inner=True):
        for zz, yes in sides(d, inner):
            @pl.when(yes & (zz >= 0) & (zz < line) & plain(zz, i))
            def _():
                c, u = item(core, i)
                slot = at(zz, 1 - y, c) * units + u
                arrived(slot)
                unit_copy(slot, (zz * 2 + 1 - y) * units + i, 3, sibling).start()
                keep(slot)

    def beside(d, aside, i, inner=True):
        c, u = item(1 - core, i)
        for zz, yes in sides(d, inner):
            there = yes & (zz >= 0) & (zz < line)
            if not aside:
                there &= (d > 0) | (c != core)

            @pl.when(there)
            def _():
                yy = 1 - y if aside else y
                slot = at(zz, yy, c) * units + u
                arrived(slot)
                keep(slot)

    def each(c, path, body, lo=0, hi=None):
        if units > 1:
            pl.loop(c * span + lo, c * span + (span if hi is None else hi))(body)
        elif lo == 0:
            pl.when(path == c)(lambda: body(jnp.int32(0)))

    def cross_owner(d, c, lo=0, hi=None):
        each(c, core, lambda i: cross(jnp.int32(d), i), lo, hi)

    def along_owner(d, c, lo=0, hi=None):
        each(c, core, lambda i: along(jnp.int32(d), i), lo, hi)

    def beside_owner(d, aside, c):
        each(c, 1 - core, lambda i: beside(jnp.int32(d), aside, i))

    per = units + 1

    def crossing_unit():
        @pl.when(detoured(z))
        def _():
            slot, _, _ = slot_of(z, jnp.int32(units))
            arrived(slot)
            forward(z, jnp.int32(units))
            keep(slot)

    def prepare(row):
        q_ref[row] = raw_q[row].T
        total_ref[pl.ds(row * heads, heads)] = jnp.zeros((heads, 1), jnp.float32)
        top_ref[pl.ds(row * heads, heads)] = jnp.full((heads, 1), HIDDEN, jnp.float32)
        acc_ref[pl.ds(row * heads, heads)] = jnp.zeros((heads, LAT), jnp.float32)

    scale = SOFTMAX_SCALE * LOG2E
    deep = CHUNK * BLOCK
    rowset = 4 if rows % 4 == 0 else 1
    groups = rows // rowset
    height = rowset * heads
    parts = 2 if rowset % 2 == 0 else 1

    def fill(n):
        places = []
        for k in range(CHUNK):
            p, slot = listed[n * CHUNK + k, 0], listed[n * CHUNK + k, 1]
            here = slice(k * BLOCK, (k + 1) * BLOCK)
            keys[here, :LAT] = pool[p // owned * (2 * units) + slot]
            both = tails[p // owned * units + slot // 2]
            tail = jnp.where(lax.rem(slot, 2) == 0, both[:, : LAT // 2], both[:, LAT // 2 :])
            keys[here, LAT:] = jnp.concatenate(
                [tail[:, i * rope : (i + 1) * rope] for i in range(BLOCK // tall)], axis=0
            )
            places.append(p * BLOCK)
        for k in range(0, CHUNK, 2):
            positions[:, k * BLOCK : (k + 2) * BLOCK] = jnp.where(
                lane < BLOCK, places[k] + lane, places[k + 1] + lane - BLOCK
            )

    def qk(g, s_ref):
        for t in range(parts):
            low, many = g * rowset + t * rowset // parts, rowset // parts
            s_ref[t * height // parts : (t + 1) * height // parts] = lax.dot_general(
                q_ref[low : low + many].reshape(many * heads, feature), keys[...],
                (((1,), (1,)), ((), ())), preferred_element_type=jnp.float32,
            )

    def soft(g, s_ref, p_ref, h_ref):
        span_g = slice(g * height, (g + 1) * height)
        where = positions[...]
        s = jnp.concatenate(
            [
                jnp.where(
                    where < lengths_ref[g * rowset + r], s_ref[r * heads : (r + 1) * heads], HIDDEN
                )
                for r in range(rowset)
            ],
            axis=0,
        )
        before = top_ref[span_g]
        top = jnp.maximum(before, jnp.max(s, axis=1, keepdims=True))
        e = jnp.exp2((s - top) * scale)
        shrink = jnp.exp2((before - top) * scale)
        total_ref[span_g] = total_ref[span_g] * shrink + jnp.sum(e, axis=1, keepdims=True)
        top_ref[span_g] = top
        p_ref[...] = e.astype(jnp.bfloat16)
        h_ref[...] = shrink

    def pv(g, p_ref, h_ref, final):
        span_g = slice(g * height, (g + 1) * height)
        o = acc_ref[span_g] * h_ref[...] + jnp.dot(
            p_ref[...], keys[:, :LAT], preferred_element_type=jnp.float32
        )
        if final:
            o = (o * (1.0 / total_ref[span_g])).astype(jnp.bfloat16)
            out_ref[g * rowset : (g + 1) * rowset] = o.reshape(rowset, heads, LAT)
        else:
            acc_ref[span_g] = o

    def attend(n, final=False):
        fill(n)
        s, p, h = (s_a, s_b), (p_a, p_b), (h_a, h_b)
        for g in range(groups + 2):
            if g < groups:
                qk(g, s[g % 2])
            if 1 <= g <= groups:
                soft(g - 1, s[(g - 1) % 2], p[(g - 1) % 2], h[(g - 1) % 2])
            if g >= 2:
                pv(g - 2, p[g % 2], h[g % 2], final)

    def generic():
        main = per * (line - 2)
        share = -(-rows // main)

        @pl.loop(0, main)
        def _(k):
            d = k // per + 1
            j = lax.rem(k, per)
            along(d, j)

            pl.when(k == span)(crossing_unit)

            @pl.when(j < units)
            def _():
                cross(d - 1, j)
                beside(d - 1, False, j)

            @pl.when((j < units) & (d > 1))
            def _():
                beside(d - 2, True, j)

            for r in range(share):
                @pl.when(k * share + r < rows)
                def _():
                    prepare(lax.rem(k * share + r, rows))

        @pl.loop(0, units)
        def _(i):
            beside(jnp.int32(line - 2), False, i)
            beside(jnp.int32(line - 3), True, i)

        ready = [(TOPK - (6 - v) * units) // CHUNK for v in range(7)]

        def attend_ready(v, lo=None, hi=None):
            lo = (ready[v - 1] if v else 0) if lo is None else lo
            hi = min(ready[v], TOPK // CHUNK - 1) if hi is None else hi
            if hi - lo == 1:
                attend(lo)
            elif hi > lo:
                pl.loop(lo, hi)(lambda n: attend(n))

        attend_ready(0, hi=1)
        cross_owner(line - 2, 0)
        attend_ready(0, lo=1)
        along_owner(line - 1, 0, 0, 1)
        beside_owner(line - 2, True, 0)
        attend_ready(1)
        cross_owner(line - 2, 1)
        along_owner(line - 1, 0, 1)
        beside_owner(line - 2, True, 1)
        attend_ready(2)
        along_owner(line - 1, 1, 0, 1)
        cross_owner(line - 1, 0, 0, 1)
        beside_owner(line - 1, False, 0)
        attend_ready(3)
        cross_owner(line - 1, 0, 1)
        along_owner(line - 1, 1, 1)
        beside_owner(line - 1, True, 0)
        attend_ready(4)
        along(jnp.int32(line - 1), jnp.int32(units))
        cross_owner(line - 1, 1, 0, 1)
        beside_owner(line - 1, False, 1)
        attend_ready(5)
        cross_owner(line - 1, 1, 1)
        beside_owner(line - 1, True, 1)
        attend(TOPK // CHUNK - 1, final=True)

    def perform(work, inner):
        for w in work:
            kind, d, i = w // 100, w // 10 % 10, jnp.int32(w % 10)
            if kind == 1:
                along(d, i, inner)
            elif kind == 2:
                cross(d, i, inner)
            elif kind in (3, 4):
                beside(d, kind == 4, i, inner)
            elif kind == 5:
                crossing_unit()

    def preparation(work, before):
        shares = EDGE.count(600)
        pl.loop(before * rows // shares, (before + work) * rows // shares)(prepare)

    def pieces(work, chunk):
        starts = [0] + [work.index(700 + n) + 1 for n in range(8)]
        return work[starts[chunk] : starts[chunk + 1] - 1]

    def emit(work, inner):
        done, batch = 0, []
        for w in work + (0,):
            if w in (0, 600):
                perform(batch, inner)
                batch = []
                if w:
                    preparation(1, done)
                    done += 1
            else:
                batch.append(w)

    listing.wait()
    fetch_lengths.wait()
    if scripted:
        for n in range(8):
            pl.when(edge)(lambda: emit(pieces(EDGE, n), False))
            pl.when(jnp.logical_not(edge))(lambda: emit(pieces(INNER, n), True))
            attend(n, final=n == 7)
    else:
        generic()

    @pl.loop(1, ctx_count)
    def _(d):
        flag_copy(d).wait_send()

    @pl.loop(0, per * line)
    def _(k):
        zz = k // per
        j = lax.rem(k, per)
        slot, local, c = slot_of(zz, j)
        for way, target, yes in sends(zz, j, c):
            @pl.when(yes)
            def _():
                unit_copy(slot, local, way, target).wait_send()

    @pl.loop(0, units * line)
    def _(k):
        zz = k // units
        i = lax.rem(k, units)

        @pl.when(plain(zz, i))
        def _():
            c, u = item(core, i)
            slot = at(zz, 1 - y, c) * units + u
            unit_copy(slot, (zz * 2 + 1 - y) * units + i, 3, sibling).wait_send()

    if units > 1:
        for u in range(units):
            @pl.when(core != u // span)
            def _():
                unit_copy(me * units + u, other_path(u), 3, sibling).wait_send()


def shards(queries, latent_cache, block_picks, lengths):
    ctx_count = lax.axis_size("ctx")
    rows, heads, feature = queries.shape
    owned = latent_cache.shape[0] // BLOCK
    units = max(1, 2 * TOPK // ctx_count)
    flag_rows = -(-(ctx_count * owned) // LANES)
    tall = 2 * BLOCK + 2 * BLOCK * (feature - LAT) // LAT
    height = (4 if rows % 4 == 0 else 1) * heads
    return pl.pallas_call(
        functools.partial(step_kernel, ctx_count, owned, units),
        out_shape=pltpu.VMEM((rows, heads, LAT), jnp.bfloat16),
        in_specs=[
            pl.BlockSpec(memory_space=pl.ANY),
            pl.BlockSpec(memory_space=pl.ANY),
            pl.BlockSpec(memory_space=pl.ANY),
            pl.BlockSpec(memory_space=pl.ANY),
        ],
        out_specs=pl.BlockSpec(memory_space=pltpu.VMEM),
        scratch_shapes=[
            pltpu.SMEM((1, TOPK), jnp.int32),
            pltpu.SMEM((rows,), jnp.int32),
            pltpu.VMEM((rows, feature, heads), jnp.bfloat16),
            pltpu.VMEM((feature, owned * BLOCK), jnp.bfloat16),
            pltpu.VMEM((owned, BLOCK, LAT), jnp.bfloat16),
            pltpu.VMEM((owned, tall - 2 * BLOCK, LAT // 2), jnp.bfloat16),
            pltpu.VMEM((rows, heads, feature), jnp.bfloat16),
            pltpu.VMEM((flag_rows, LANES), jnp.int32),
            pltpu.VMEM((ctx_count, flag_rows, LANES), jnp.int32),
            pltpu.VMEM((ctx_count * units, tall, LAT), jnp.bfloat16),
            pltpu.VMEM((ctx_count * units * 2, BLOCK, LAT), jnp.bfloat16),
            pltpu.VMEM((ctx_count * units, tall - 2 * BLOCK, LAT), jnp.bfloat16),
            pltpu.VMEM((CHUNK * BLOCK, feature), jnp.bfloat16),
            pltpu.VMEM((1, CHUNK * BLOCK), jnp.int32),
            pltpu.VMEM((TOPK, LANES), jnp.int32),
            pltpu.SMEM((TOPK, LANES), jnp.int32),
            pltpu.VMEM((rows * heads, 1), jnp.float32),
            pltpu.VMEM((rows * heads, 1), jnp.float32),
            pltpu.VMEM((rows * heads, LAT), jnp.float32),
            *[pltpu.VMEM((height, CHUNK * BLOCK), jnp.float32)] * 2,
            *[pltpu.VMEM((height, CHUNK * BLOCK), jnp.bfloat16)] * 2,
            *[pltpu.VMEM((height, 1), jnp.float32)] * 2,
            *[pltpu.SemaphoreType.DMA] * 5,
            pltpu.SemaphoreType.DMA((ctx_count,)),
            pltpu.SemaphoreType.DMA((ctx_count,)),
            pltpu.SemaphoreType.DMA((ctx_count // 2 * units, 4)),
            pltpu.SemaphoreType.DMA((ctx_count * units,)),
        ],
        compiler_params=pltpu.CompilerParams(
            collective_id=0, has_side_effects=True, vmem_limit_bytes=64_900_000
        ),
    )(block_picks, lengths, jnp.swapaxes(queries, 1, 2), latent_cache.T)


def solution(mesh):
    placed = (
        P(("groups", "ctx"), None, None),
        P(("groups", "ctx"), None),
        P(("groups", "ctx"), None),
        P(("groups", "ctx")),
    )
    return jax.shard_map(
        shards,
        mesh=mesh,
        in_specs=placed,
        out_specs=P(("groups", "ctx"), None, None),
        check_vma=False,
    )
```

```python
import functools

import jax
import jax.numpy as jnp
from jax import lax
from jax.experimental import pallas as pl
from jax.experimental.pallas import tpu as pltpu
from jax.sharding import PartitionSpec as P

LAT = 512
BLOCK = 64
TOPK = 32
LANES = 128

SOFTMAX_SCALE = 192.0 ** (-0.5)
LOG2E = 1.4426950408889634
MESH = pl.DeviceIdType.MESH
HIDDEN = -1e30
CHUNK = 4

EDGE = (
    111, 110, 300, 500, 112, 600, 311, 113, 310, 203, 120, 320, 302, 210, 201, 122, 313, 303,
    402, 312, 202, 211, 213, 121, 200, 411, 600, 413, 114, 403, 401, 123, 212, 600, 600, 301,
    321, 410, 400, 412, 222, 322, 220, 700, 124, 323, 420, 130, 232, 221, 701, 223, 131, 421,
    330, 422, 702, 423, 331, 230, 703, 133, 430, 231, 704, 132, 431, 705, 233, 333, 332, 134,
    706, 433, 432, 707,
)
INNER = (
    303, 110, 112, 111, 500, 210, 312, 113, 410, 600, 310, 114, 200, 202, 212, 120, 201, 302,
    402, 211, 600, 401, 203, 121, 320, 301, 600, 321, 123, 313, 300, 122, 403, 600, 311, 400,
    323, 411, 700, 322, 124, 213, 701, 412, 413, 702, 703, 223, 222, 422, 220, 221, 704, 421,
    420, 705, 423, 706, 707,
)


def step_kernel(
    ctx_count, owned, units, picks_hbm, lengths_hbm, queries_ref, cache_ref, out_ref,
    picks_ref, lengths_ref, raw_q, near_cache, near, near_tails, q_ref, flags_ref, all_flags, gath, pool, tails, keys, positions, listed_v, listed,
    top_ref, total_ref, acc_ref, s_a, s_b, p_a, p_b, h_a, h_b,
    picks_sem, lengths_sem, q_sem, cache_sem, list_sem, flag_send, flag_recv, send, recv,
):
    rows, feature, heads = queries_ref.shape
    rope = feature - LAT
    pair = 2 * BLOCK
    tall = pair * rope // LAT
    line = ctx_count // 4
    span = max(1, units // 2)
    crossing = span if units > 1 else 0
    me = lax.axis_index("ctx")
    core = lax.rem(me, 2)
    y = lax.rem(me // 2, 2)
    z = me // 4

    fetch = pltpu.make_async_copy(queries_ref, raw_q, q_sem)
    fetch_cache = pltpu.make_async_copy(cache_ref, near_cache, cache_sem)
    fetch_picks = pltpu.make_async_copy(picks_hbm, picks_ref, picks_sem)
    fetch_lengths = pltpu.make_async_copy(lengths_hbm, lengths_ref, lengths_sem)
    fetch_picks.start()

    def at(zz, yy, cc):
        return (zz * 2 + yy) * 2 + cc

    barrier = pltpu.get_barrier_semaphore()

    @pl.loop(1, ctx_count, unroll=ctx_count - 1 < 16)
    def _(d):
        pl.semaphore_signal(
            barrier, inc=1, device_id={"ctx": lax.rem(me + d, ctx_count)}, device_id_type=MESH
        )

    fetch_cache.start()
    fetch_lengths.start()
    fetch.start()
    fetch_picks.wait()
    flag_rows = flags_ref.shape[0]
    block_id = lax.broadcasted_iota(jnp.int32, (flag_rows, LANES), 0) * LANES
    block_id += lax.broadcasted_iota(jnp.int32, (flag_rows, LANES), 1)
    lane = lax.broadcasted_iota(jnp.int32, (1, LANES), 1)
    flags = jnp.zeros((flag_rows, LANES), jnp.int32)
    for k in range(TOPK):
        flags = jnp.where(block_id == picks_ref[0, k], 1, flags)
    flags_ref[...] = flags

    pl.semaphore_wait(barrier, ctx_count - 1)

    def flag_copy(d):
        return pltpu.make_async_remote_copy(
            src_ref=flags_ref,
            dst_ref=all_flags.at[me],
            send_sem=flag_send.at[d],
            recv_sem=flag_recv.at[me],
            device_id={"ctx": lax.rem(me + d, ctx_count)},
            device_id_type=MESH,
        )

    def flag_arrival(source):
        return pltpu.make_async_remote_copy(
            src_ref=flags_ref,
            dst_ref=all_flags.at[source],
            send_sem=flag_send.at[0],
            recv_sem=flag_recv.at[source],
            device_id={"ctx": source},
            device_id_type=MESH,
        )

    @pl.loop(1, ctx_count, unroll=ctx_count - 1 < 16)
    def _(d):
        flag_copy(d).start()

    all_flags[me] = flags

    scripted = line == 4 and units == 4 and TOPK // CHUNK == 8
    edge = (z == 0) | (z == line - 1)

    def stage(p):
        owner = p // owned
        away = jnp.abs(owner // 4 - z)
        aside = (lax.rem(owner // 2, 2) != y).astype(jnp.int32)
        c = lax.rem(owner, 2)
        if scripted:
            near = jnp.where(aside == 1, 2 + c, c)
            outer = jnp.where(away == 3, 4 + 2 * c + aside, jnp.where(away == 2, near, 0))
            near = jnp.where(away == 1, aside * (2 + 2 * c), 0)
            return jnp.where(edge, outer, jnp.where(away == 2, aside * 6 + c, near))
        last = 3 + 2 * c + aside
        return jnp.where(away == line - 1, last, jnp.where(away == line - 2, aside * (1 + c), 0))

    stages = [stage(picks_ref[0, k]) for k in range(TOPK)]
    begin, total = [], jnp.int32(0)
    for v in range(8):
        begin.append(total)
        for k in range(TOPK):
            total += (stages[k] == v).astype(jnp.int32)
    ordered = jnp.zeros((1, LANES), jnp.int32)
    for k in range(TOPK):
        place = jnp.int32(0)
        for v in range(8):
            here = (stages[k] == v).astype(jnp.int32)
            place += here * begin[v]
            begin[v] += here
        ordered = jnp.where(lane == place, picks_ref[0, k], ordered)

    fetch_cache.wait()

    @pl.loop(0, owned // 2)
    def _(b):
        tokens = near_cache[:, pl.ds(pl.multiple_of(b * pair, pair), pair)].T
        tail = tokens[:, LAT:]
        packed = jnp.concatenate(
            [tail[i * tall : (i + 1) * tall, :] for i in range(pair // tall)], axis=1
        )
        near[2 * b] = tokens[:BLOCK, :LAT]
        near[2 * b + 1] = tokens[BLOCK:, :LAT]
        near_tails[2 * b] = packed[:, : LAT // 2]
        near_tails[2 * b + 1] = packed[:, LAT // 2 :]

    @pl.loop(1, ctx_count)
    def _(d):
        flag_arrival(lax.rem(me + d, ctx_count)).wait_recv()

    named = jnp.minimum(jnp.max(all_flags[...], axis=0), 1)
    mine = (named > 0) & (block_id // owned == me)

    def unit_copy(slot, local, way, target):
        return pltpu.make_async_remote_copy(
            src_ref=gath.at[slot],
            dst_ref=gath.at[slot],
            send_sem=send.at[local, way],
            recv_sem=recv.at[slot],
            device_id={"ctx": target},
            device_id_type=MESH,
        )

    def item(path, i):
        if units > 1:
            return i // span, path * span + lax.rem(i, span)
        return path, i * 0

    def detoured(zz):
        if units > 1:
            return (core == 1) | (zz == 0) | (zz == line - 1)
        return core == 1

    def plain(zz, i):
        return jnp.logical_not(detoured(zz)) | (i != crossing)

    def slot_of(zz, j):
        crossed = (j == units).astype(jnp.int32)
        i = jnp.where(j == units, crossing, j)
        yy = lax.rem(y + crossed, 2)
        c, u = item(core, i)
        return at(zz, yy, c) * units + u, (zz * 2 + yy) * units + i, c

    up = at(lax.rem(z + 1, line), y, core)
    down = at(lax.rem(z + line - 1, line), y, core)
    across = at(z, 1 - y, core)
    sibling = at(z, y, 1 - core)

    def sends(zz, j, c):
        valid = (zz >= 0) & (zz < line) & ((j < units) | detoured(zz))
        own_line = j < units
        return (
            (0, up, valid & (zz <= z) & (z + 1 < line)),
            (1, down, valid & (zz >= z) & (z > 0)),
            (2, across, valid & own_line & ((zz == z) | plain(zz, j))),
            (3, sibling, valid & ((zz != z) | (j == units) | (c == core))),
        )

    def forward(zz, j, skip=()):
        slot, local, c = slot_of(zz, j)
        for way, target, yes in sends(zz, j, c):
            if way not in skip:
                @pl.when(yes)
                def _():
                    unit_copy(slot, local, way, target).start()

    def arrived(slot):
        unit_copy(slot, 0, 0, sibling).wait_recv()

    def keep(slot):
        pool[2 * slot] = gath[slot, :BLOCK]
        pool[2 * slot + 1] = gath[slot, BLOCK:pair]
        tails[slot] = gath[slot, pair:]

    past = ctx_count * owned
    starts = []
    last = jnp.int32(-1)

    def other_path(u):
        return (z * 2 + y) * units + (1 - core) * span + u % span

    for u in [v for r in range(span) for v in range(r, units, span)]:
        while len(starts) < 2 * u + 2:
            last = jnp.min(jnp.where(mine & (block_id > last), block_id, past))
            starts.append(jnp.minimum(last - me * owned, owned - 1))
        unit = me * units + u
        for h in range(2):
            block = starts[2 * u + h]
            gath[unit, h * BLOCK : (h + 1) * BLOCK, :] = near[block]
            gath[unit, pair:, h * LAT // 2 : (h + 1) * LAT // 2] = near_tails[block]
        if units == 1:
            forward(z, jnp.int32(0))
        else:
            path = u // span
            position = jnp.int32(path * span + u % span)

            @pl.when((core == path) & (core == 0))
            def _():
                forward(z, position)

            @pl.when((core == path) & (core == 1))
            def _():
                forward(z, position, (0, 1, 2))

            @pl.when(core != path)
            def _():
                unit_copy(me * units + u, other_path(u), 3, sibling).start()

    @pl.loop(0, units)
    def _(u):
        keep(me * units + u)

    if units > 1:
        @pl.loop(0, units)
        def _(i):
            slot, _, c = slot_of(z, i)

            @pl.when(c != core)
            def _():
                arrived(slot)
                forward(z, i)
                keep(slot)

            @pl.when((c == core) & (core == 1))
            def _():
                forward(z, i, (3,))

    fetch.wait()

    within = lax.rem(block_id, owned)
    before = named
    shift = 1
    while shift < owned:
        before += jnp.where(within >= shift, pltpu.roll(before, shift, 1), 0)
        shift *= 2
    before -= named
    wide = lax.broadcasted_iota(jnp.int32, (TOPK, LANES), 1)
    tall_id = lax.broadcasted_iota(jnp.int32, (TOPK, LANES), 0)
    column_p = jnp.sum(jnp.where(wide == tall_id, ordered, 0), axis=1, keepdims=True)
    found = jnp.zeros((TOPK, LANES), jnp.int32)
    for r in range(-(-past // LANES)):
        found += jnp.where(column_p == wide + r * LANES, before[r : r + 1, :], 0)
    column_s = jnp.sum(found, axis=1, keepdims=True)
    listed_v[...] = jnp.where(wide == 0, column_p, column_s)
    listing = pltpu.make_async_copy(listed_v, listed, list_sem)
    listing.start()

    def sides(d, inner=True):
        if not scripted:
            return ((z + d, d >= 0), (z - d, d > 0))
        if inner and d == 1:
            return ((z + 1, True), (z - 1, True))
        return ((jnp.where(z + d < line, z + d, z - d), True),)

    def along(d, j, inner=True):
        for zz, yes in sides(d, inner):
            @pl.when(yes & (zz >= 0) & (zz < line) & ((j < units) | detoured(zz)))
            def _():
                slot, _, _ = slot_of(zz, j)
                arrived(slot)
                forward(zz, j)
                keep(slot)

    def cross(d, i, inner=True):
        for zz, yes in sides(d, inner):
            @pl.when(yes & (zz >= 0) & (zz < line) & plain(zz, i))
            def _():
                c, u = item(core, i)
                slot = at(zz, 1 - y, c) * units + u
                arrived(slot)
                unit_copy(slot, (zz * 2 + 1 - y) * units + i, 3, sibling).start()
                keep(slot)

    def beside(d, aside, i, inner=True):
        c, u = item(1 - core, i)
        for zz, yes in sides(d, inner):
            there = yes & (zz >= 0) & (zz < line)
            if not aside:
                there &= (d > 0) | (c != core)

            @pl.when(there)
            def _():
                yy = 1 - y if aside else y
                slot = at(zz, yy, c) * units + u
                arrived(slot)
                keep(slot)

    def each(c, path, body, lo=0, hi=None):
        if units > 1:
            pl.loop(c * span + lo, c * span + (span if hi is None else hi))(body)
        elif lo == 0:
            pl.when(path == c)(lambda: body(jnp.int32(0)))

    def cross_owner(d, c, lo=0, hi=None):
        each(c, core, lambda i: cross(jnp.int32(d), i), lo, hi)

    def along_owner(d, c, lo=0, hi=None):
        each(c, core, lambda i: along(jnp.int32(d), i), lo, hi)

    def beside_owner(d, aside, c):
        each(c, 1 - core, lambda i: beside(jnp.int32(d), aside, i))

    per = units + 1

    def crossing_unit():
        @pl.when(detoured(z))
        def _():
            slot, _, _ = slot_of(z, jnp.int32(units))
            arrived(slot)
            forward(z, jnp.int32(units))
            keep(slot)

    def prepare(row):
        q_ref[row] = raw_q[row].T
        total_ref[pl.ds(row * heads, heads)] = jnp.zeros((heads, 1), jnp.float32)
        top_ref[pl.ds(row * heads, heads)] = jnp.full((heads, 1), HIDDEN, jnp.float32)
        acc_ref[pl.ds(row * heads, heads)] = jnp.zeros((heads, LAT), jnp.float32)

    scale = SOFTMAX_SCALE * LOG2E
    deep = CHUNK * BLOCK
    rowset = 4 if rows % 4 == 0 else 1
    groups = rows // rowset
    height = rowset * heads
    parts = 2 if rowset % 2 == 0 else 1

    def fill(n):
        places = []
        for k in range(CHUNK):
            p, slot = listed[n * CHUNK + k, 0], listed[n * CHUNK + k, 1]
            here = slice(k * BLOCK, (k + 1) * BLOCK)
            keys[here, :LAT] = pool[p // owned * (2 * units) + slot]
            both = tails[p // owned * units + slot // 2]
            tail = jnp.where(lax.rem(slot, 2) == 0, both[:, : LAT // 2], both[:, LAT // 2 :])
            keys[here, LAT:] = jnp.concatenate(
                [tail[:, i * rope : (i + 1) * rope] for i in range(BLOCK // tall)], axis=0
            )
            places.append(p * BLOCK)
        for k in range(0, CHUNK, 2):
            positions[:, k * BLOCK : (k + 2) * BLOCK] = jnp.where(
                lane < BLOCK, places[k] + lane, places[k + 1] + lane - BLOCK
            )

    def qk(g, s_ref):
        for t in range(parts):
            low, many = g * rowset + t * rowset // parts, rowset // parts
            s_ref[t * height // parts : (t + 1) * height // parts] = lax.dot_general(
                q_ref[low : low + many].reshape(many * heads, feature), keys[...],
                (((1,), (1,)), ((), ())), preferred_element_type=jnp.float32,
            )

    def soft(g, s_ref, p_ref, h_ref):
        span_g = slice(g * height, (g + 1) * height)
        where = positions[...]
        s = jnp.concatenate(
            [
                jnp.where(
                    where < lengths_ref[g * rowset + r], s_ref[r * heads : (r + 1) * heads], HIDDEN
                )
                for r in range(rowset)
            ],
            axis=0,
        )
        before = top_ref[span_g]
        top = jnp.maximum(before, jnp.max(s, axis=1, keepdims=True))
        e = jnp.exp2((s - top) * scale)
        shrink = jnp.exp2((before - top) * scale)
        total_ref[span_g] = total_ref[span_g] * shrink + jnp.sum(e, axis=1, keepdims=True)
        top_ref[span_g] = top
        p_ref[...] = e.astype(jnp.bfloat16)
        h_ref[...] = shrink

    def pv(g, p_ref, h_ref, final):
        span_g = slice(g * height, (g + 1) * height)
        o = acc_ref[span_g] * h_ref[...] + jnp.dot(
            p_ref[...], keys[:, :LAT], preferred_element_type=jnp.float32
        )
        if final:
            o = (o * (1.0 / total_ref[span_g])).astype(jnp.bfloat16)
            out_ref[g * rowset : (g + 1) * rowset] = o.reshape(rowset, heads, LAT)
        else:
            acc_ref[span_g] = o

    def attend(n, final=False):
        fill(n)
        s, p, h = (s_a, s_b), (p_a, p_b), (h_a, h_b)
        for g in range(groups + 2):
            if g < groups:
                qk(g, s[g % 2])
            if 1 <= g <= groups:
                soft(g - 1, s[(g - 1) % 2], p[(g - 1) % 2], h[(g - 1) % 2])
            if g >= 2:
                pv(g - 2, p[g % 2], h[g % 2], final)

    def generic():
        main = per * (line - 2)
        share = -(-rows // main)

        @pl.loop(0, main)
        def _(k):
            d = k // per + 1
            j = lax.rem(k, per)
            along(d, j)

            pl.when(k == span)(crossing_unit)

            @pl.when(j < units)
            def _():
                cross(d - 1, j)
                beside(d - 1, False, j)

            @pl.when((j < units) & (d > 1))
            def _():
                beside(d - 2, True, j)

            for r in range(share):
                @pl.when(k * share + r < rows)
                def _():
                    prepare(lax.rem(k * share + r, rows))

        @pl.loop(0, units)
        def _(i):
            beside(jnp.int32(line - 2), False, i)
            beside(jnp.int32(line - 3), True, i)

        ready = [(TOPK - (6 - v) * units) // CHUNK for v in range(7)]

        def attend_ready(v, lo=None, hi=None):
            lo = (ready[v - 1] if v else 0) if lo is None else lo
            hi = min(ready[v], TOPK // CHUNK - 1) if hi is None else hi
            if hi - lo == 1:
                attend(lo)
            elif hi > lo:
                pl.loop(lo, hi)(lambda n: attend(n))

        attend_ready(0, hi=1)
        cross_owner(line - 2, 0)
        attend_ready(0, lo=1)
        along_owner(line - 1, 0, 0, 1)
        beside_owner(line - 2, True, 0)
        attend_ready(1)
        cross_owner(line - 2, 1)
        along_owner(line - 1, 0, 1)
        beside_owner(line - 2, True, 1)
        attend_ready(2)
        along_owner(line - 1, 1, 0, 1)
        cross_owner(line - 1, 0, 0, 1)
        beside_owner(line - 1, False, 0)
        attend_ready(3)
        cross_owner(line - 1, 0, 1)
        along_owner(line - 1, 1, 1)
        beside_owner(line - 1, True, 0)
        attend_ready(4)
        along(jnp.int32(line - 1), jnp.int32(units))
        cross_owner(line - 1, 1, 0, 1)
        beside_owner(line - 1, False, 1)
        attend_ready(5)
        cross_owner(line - 1, 1, 1)
        beside_owner(line - 1, True, 1)
        attend(TOPK // CHUNK - 1, final=True)

    def perform(work, inner):
        for w in work:
            kind, d, i = w // 100, w // 10 % 10, jnp.int32(w % 10)
            if kind == 1:
                along(d, i, inner)
            elif kind == 2:
                cross(d, i, inner)
            elif kind in (3, 4):
                beside(d, kind == 4, i, inner)
            elif kind == 5:
                crossing_unit()

    def preparation(work, before):
        shares = EDGE.count(600)
        pl.loop(before * rows // shares, (before + work) * rows // shares)(prepare)

    def pieces(work, chunk):
        starts = [0] + [work.index(700 + n) + 1 for n in range(8)]
        return work[starts[chunk] : starts[chunk + 1] - 1]

    def emit(work, inner):
        done, batch = 0, []
        for w in work + (0,):
            if w in (0, 600):
                perform(batch, inner)
                batch = []
                if w:
                    preparation(1, done)
                    done += 1
            else:
                batch.append(w)

    listing.wait()
    fetch_lengths.wait()
    if scripted:
        for n in range(8):
            pl.when(edge)(lambda: emit(pieces(EDGE, n), False))
            pl.when(jnp.logical_not(edge))(lambda: emit(pieces(INNER, n), True))
            attend(n, final=n == 7)
    else:
        generic()

    @pl.loop(1, ctx_count)
    def _(d):
        flag_copy(d).wait_send()

    @pl.loop(0, per * line)
    def _(k):
        zz = k // per
        j = lax.rem(k, per)
        slot, local, c = slot_of(zz, j)
        for way, target, yes in sends(zz, j, c):
            @pl.when(yes)
            def _():
                unit_copy(slot, local, way, target).wait_send()

    @pl.loop(0, units * line)
    def _(k):
        zz = k // units
        i = lax.rem(k, units)

        @pl.when(plain(zz, i))
        def _():
            c, u = item(core, i)
            slot = at(zz, 1 - y, c) * units + u
            unit_copy(slot, (zz * 2 + 1 - y) * units + i, 3, sibling).wait_send()

    if units > 1:
        for u in range(units):
            @pl.when(core != u // span)
            def _():
                unit_copy(me * units + u, other_path(u), 3, sibling).wait_send()


def shards(queries, latent_cache, block_picks, lengths):
    ctx_count = lax.axis_size("ctx")
    rows, heads, feature = queries.shape
    owned = latent_cache.shape[0] // BLOCK
    units = max(1, 2 * TOPK // ctx_count)
    flag_rows = -(-(ctx_count * owned) // LANES)
    tall = 2 * BLOCK + 2 * BLOCK * (feature - LAT) // LAT
    height = (4 if rows % 4 == 0 else 1) * heads
    return pl.pallas_call(
        functools.partial(step_kernel, ctx_count, owned, units),
        out_shape=pltpu.VMEM((rows, heads, LAT), jnp.bfloat16),
        in_specs=[
            pl.BlockSpec(memory_space=pl.ANY),
            pl.BlockSpec(memory_space=pl.ANY),
            pl.BlockSpec(memory_space=pl.ANY),
            pl.BlockSpec(memory_space=pl.ANY),
        ],
        out_specs=pl.BlockSpec(memory_space=pltpu.VMEM),
        scratch_shapes=[
            pltpu.SMEM((1, TOPK), jnp.int32),
            pltpu.SMEM((rows,), jnp.int32),
            pltpu.VMEM((rows, feature, heads), jnp.bfloat16),
            pltpu.VMEM((feature, owned * BLOCK), jnp.bfloat16),
            pltpu.VMEM((owned, BLOCK, LAT), jnp.bfloat16),
            pltpu.VMEM((owned, tall - 2 * BLOCK, LAT // 2), jnp.bfloat16),
            pltpu.VMEM((rows, heads, feature), jnp.bfloat16),
            pltpu.VMEM((flag_rows, LANES), jnp.int32),
            pltpu.VMEM((ctx_count, flag_rows, LANES), jnp.int32),
            pltpu.VMEM((ctx_count * units, tall, LAT), jnp.bfloat16),
            pltpu.VMEM((ctx_count * units * 2, BLOCK, LAT), jnp.bfloat16),
            pltpu.VMEM((ctx_count * units, tall - 2 * BLOCK, LAT), jnp.bfloat16),
            pltpu.VMEM((CHUNK * BLOCK, feature), jnp.bfloat16),
            pltpu.VMEM((1, CHUNK * BLOCK), jnp.int32),
            pltpu.VMEM((TOPK, LANES), jnp.int32),
            pltpu.SMEM((TOPK, LANES), jnp.int32),
            pltpu.VMEM((rows * heads, 1), jnp.float32),
            pltpu.VMEM((rows * heads, 1), jnp.float32),
            pltpu.VMEM((rows * heads, LAT), jnp.float32),
            *[pltpu.VMEM((height, CHUNK * BLOCK), jnp.float32)] * 2,
            *[pltpu.VMEM((height, CHUNK * BLOCK), jnp.bfloat16)] * 2,
            *[pltpu.VMEM((height, 1), jnp.float32)] * 2,
            *[pltpu.SemaphoreType.DMA] * 5,
            pltpu.SemaphoreType.DMA((ctx_count,)),
            pltpu.SemaphoreType.DMA((ctx_count,)),
            pltpu.SemaphoreType.DMA((ctx_count // 2 * units, 4)),
            pltpu.SemaphoreType.DMA((ctx_count * units,)),
        ],
        compiler_params=pltpu.CompilerParams(
            collective_id=0, has_side_effects=True, vmem_limit_bytes=64_900_000
        ),
    )(block_picks, lengths, jnp.swapaxes(queries, 1, 2), latent_cache.T)


def solution(mesh):
    placed = (
        P(("groups", "ctx"), None, None),
        P(("groups", "ctx"), None),
        P(("groups", "ctx"), None),
        P(("groups", "ctx")),
    )
    return jax.shard_map(
        shards,
        mesh=mesh,
        in_specs=placed,
        out_specs=P(("groups", "ctx"), None, None),
        check_vma=False,
    )
```
